128 devices in a mesh: freq: 2 (over core), dir: 4 (over y), ap: 16 (over z, x).
Axes of the slice: x: 4, y: 4, z: 4, core: 2. Of those that a mesh axis runs over, the one named last changes fastest.
Arguments:
- signal: bfloat16 [2, 65536, 2048], P(None, 'ap', ('freq', 'dir')), parts along dimension 2, may hold values from -6 to 6
- positions: int32 [2, 65536], P(None, 'ap'), may hold values from 0 to 255
- weights: bfloat16 [4, 2, 2, 2, 256, 256], replicated, may hold values from -0.1875 to 0.1875
- directions: int32 [2, 16, 4096], P(None, 'ap', 'dir'), may hold values from 0 to 255
Outputs:
- beams: bfloat16 [2, 16, 4096, 2048], P(None, 'ap', 'dir', 'freq'), parts along dimension 3
The draws below stay inside these ranges and needn't reach their ends.
There are 2 independent parts, one for each index of `freq`. The reference program is written for one: setup_inputs(seed, part) draws one part's arguments, and reference() takes and returns one part's arrays. A program takes and returns all parts, laid end to end along the dimension named above; an argument that names none is the same for every part. Nothing has to cross between parts.
All inputs are finite; a program needn't handle non-finite values.
Results may differ from the reference program's by a relative error of at most 0.009.
Values may be sent and summed in bfloat16 or wider, within the bound.
No kernel may reach another device: no remote copies, remote signals or barrier semaphores. Data moves between devices by JAX's collectives and lax.ppermute only.
A program may use at most 128 MiB of HBM per device.

```python
import math
import jax
import jax.numpy as jnp
from jax import lax

K = 256
EB = 256
GRID = 256
LEVELS = 4
Q = 4096
SNAP = 32
ABOX = 16
NE = 65536
BINS = 32


def plant(values, stream_key, low, top_value):
    longest = values.shape.index(max(values.shape))
    spots = []
    for shift in (0, 1):
        where = [jax.random.randint(jax.random.fold_in(stream_key, axis), (), 0, length) for axis, length in enumerate(values.shape)]
        where[longest] = (where[longest] + shift) % values.shape[longest]
        spots.append(tuple(where))
    return values.at[spots[0]].set(low).at[spots[1]].set(top_value)


def levels(rng, dims, cuts, least, high):
    level, own = 1.0, jax.random.fold_in(rng, 6)
    for axis_at, parts in cuts:
        heights = jnp.exp(jax.random.uniform(jax.random.fold_in(own, axis_at), (parts,), jnp.float32, least / len(cuts), high / len(cuts)))
        level = level * jnp.repeat(heights, dims[axis_at] // parts).reshape([-1 if axis == axis_at else 1 for axis in range(len(dims))])
    return level


def scatter_about(stream_key, shape, scale, bound, cuts=(), held_as=jnp.bfloat16):
    drawn = jax.random.normal(stream_key, shape, jnp.float32) * scale
    if len(cuts) > 0:
        drawn = levels(stream_key, shape, cuts, -0.22, 0.18) * drawn
    return jnp.clip(drawn, min=-bound, max=bound).astype(held_as)


def setup_inputs(seed: int = 0, part: int = 0) -> dict:
    seeds = jax.random.split(jax.random.key(seed), 5)
    own_keys = jax.random.split(jax.random.fold_in(seeds[4], part), 5)
    signal = scatter_about(own_keys[0], (2, NE, BINS * SNAP), 1.0, 6.0, ((1, 16), (2, 4)))
    positions = plant(jax.random.randint(seeds[1], (2, NE), 0, GRID), jax.random.fold_in(seeds[1], 1), 0, GRID - 1).astype(jnp.int32)
    weights = scatter_about(seeds[2], (LEVELS, 2, 2, 2, K, K), (4 * K) ** -0.5, 0.1875)
    directions = plant(jax.random.randint(seeds[3], (2, ABOX, Q), 0, GRID), jax.random.fold_in(seeds[3], 1), 0, GRID - 1).astype(jnp.int32)
    return {"signal": signal, "positions": positions, "weights": weights, "directions": directions}


def rounded(values):
    return lax.optimization_barrier(values.astype(jnp.bfloat16))

def wave_table(element_x_position, coord_y, side, factor):
    wavenumber_index = jnp.arange(side * side, dtype=jnp.int32)
    wave_x = wavenumber_index // side - side // 2
    wave_y = wavenumber_index % side - side // 2
    phase_int = jnp.mod(element_x_position[..., None] * wave_x + coord_y[..., None] * wave_y, GRID)
    angle_rad = phase_int.astype(jnp.float32) * (2.0 * math.pi / GRID)
    return (jnp.cos(angle_rad) * factor, jnp.sin(angle_rad) * factor)

def group_phase(per_box, side):
    tile_rows = 1 << per_box.bit_length() // 2
    tile_columns = per_box // tile_rows
    group_index = jnp.arange(per_box, dtype=jnp.int32)
    centre_x = group_index % tile_rows * (GRID // tile_rows)
    centre_y = group_index // tile_rows * (GRID // tile_columns)
    return wave_table(centre_x, centre_y, side, 1.0)

def element_table(element_x_position, coord_y, side):
    cosine, sine_part = wave_table(element_x_position, coord_y, side, 1.0 / math.sqrt(EB))
    row_real = jnp.stack([cosine, sine_part], -3)
    row_imag = jnp.stack([-sine_part, cosine], -3)
    return jnp.stack([row_real, row_imag], -4)

def direction_table(element_x_position, coord_y, side):
    cosine, sine_part = wave_table(element_x_position, coord_y, side, 1.0 / math.sqrt(K))
    row_real = jnp.stack([cosine, -sine_part], -2)
    row_imag = jnp.stack([sine_part, cosine], -2)
    return jnp.stack([row_real, row_imag], -4)

def expand(level_pair):
    w_real = level_pair[:, 0]
    w_imag = level_pair[:, 1]
    upper_rows = jnp.stack([w_real, -w_imag], 1)
    lower_rows = jnp.stack([w_imag, w_real], 1)
    block_matrix = jnp.stack([upper_rows, lower_rows], 0).transpose(0, 3, 1, 2, 4)
    return block_matrix.reshape(2 * K, 4 * K)

def reference(signal, positions, weights, directions):
    side = math.isqrt(K)
    all_boxes = NE // EB
    columns = signal.shape[2]
    boxes_data = signal.reshape(2, all_boxes, EB, columns).transpose(1, 0, 2, 3)
    element_x_position = positions[0].reshape(all_boxes, EB)
    coord_y = positions[1].reshape(all_boxes, EB)

    def leaf_box(items):
        signal_samples, box_x, box_y = items
        phase_table = rounded(element_table(box_x, box_y, side))
        beam_output = jnp.einsum('vdhn,dhy->vny', phase_table.astype(jnp.float32), signal_samples.astype(jnp.float32))
        return rounded(beam_output)
    coeffs = lax.map(leaf_box, (boxes_data, element_x_position, coord_y))
    for level_id in range(LEVELS):
        stride = all_boxes >> level_id + 1
        grouped_boxes = coeffs.astype(jnp.float32).reshape(all_boxes // (2 * stride), 2, stride, 2 * K, columns)
        joined = grouped_boxes.transpose(0, 2, 1, 3, 4).reshape(all_boxes // (2 * stride), stride, 4 * K, columns)
        results = []
        for parity in range(2):
            block_matrix = expand(weights[level_id, parity]).astype(jnp.float32)
            results.append(jnp.einsum('ij,ghjc->ghic', block_matrix, joined))
        coeffs = rounded(jnp.stack(results, 1).reshape(all_boxes, 2, K, columns))
    per_box = all_boxes // ABOX
    cosine, sine_part = group_phase(per_box, side)
    cosine = cosine[:, :, None]
    sine_part = sine_part[:, :, None]
    grouped_boxes = coeffs.astype(jnp.float32).reshape(ABOX, per_box, 2, K, columns)
    real_part = grouped_boxes[:, :, 0] * cosine + grouped_boxes[:, :, 1] * sine_part
    imag_part = grouped_boxes[:, :, 1] * cosine - grouped_boxes[:, :, 0] * sine_part
    summed = jnp.stack([lax.optimization_barrier(jnp.sum(real_part, axis=1)), lax.optimization_barrier(jnp.sum(imag_part, axis=1))], 1)
    summed = rounded(summed * (1.0 / math.sqrt(per_box)))

    def evaluate_box(items):
        coeff_box, steer_x, steer_y = items
        phase_table = rounded(direction_table(steer_x, steer_y, side))
        beam_output = jnp.einsum('oqik,ikc->oqc', phase_table.astype(jnp.float32), coeff_box.astype(jnp.float32))
        return beam_output.astype(jnp.bfloat16)
    beam_values = lax.map(evaluate_box, (summed, directions[0], directions[1]))
    return beam_values.transpose(1, 0, 2, 3)
```

```python
import math

import jax
import jax.numpy as jnp
from jax import lax
from jax.experimental import pallas as pl
from jax.experimental.pallas import tpu as pltpu
from jax.sharding import Mesh, PartitionSpec as P

K = 256
EB = 256
SIDE = 16
BOXES = 16
HALF = 128
NH = 2
F32 = jnp.float32
BF = jnp.bfloat16


def sincos(phase):
    p = jnp.bitwise_and(phase, 255)
    q = jnp.right_shift(p + 32, 6)
    t = (p - jnp.left_shift(q, 6)).astype(F32) * (2.0 * math.pi / 256.0)
    u = t * t
    s0 = t * (1.0 + u * (-1.0 / 6 + u * (1.0 / 120 + u * (-1.0 / 5040 + u * (1.0 / 362880)))))
    c0 = 1.0 + u * (-0.5 + u * (1.0 / 24 + u * (-1.0 / 720 + u * (1.0 / 40320))))
    odd = jnp.bitwise_and(q, 1) == 1
    c = jnp.where(odd, s0, c0)
    s = jnp.where(odd, c0, s0)
    c = jnp.where(jnp.bitwise_and(q + 1, 2) == 2, -c, c)
    s = jnp.where(jnp.bitwise_and(q, 2) == 2, -s, s)
    return c, s


def dot(a, b):
    return jnp.dot(a, b, preferred_element_type=F32)


def place(offset):
    return jnp.where(offset == 0, 3, jnp.where(offset == 2, 0, jnp.where(offset == 1, 1, 2)))


def dft4(x):
    (a, b), (c, d), (e, f), (g, h) = x
    s0r, s0i, d0r, d0i = a + e, b + f, a - e, b - f
    s1r, s1i, d1r, d1i = c + g, d + h, c - g, d - h
    return (
        (s0r + s1r, s0i + s1i),
        (d0r + d1i, d0i - d1r),
        (s0r - s1r, s0i - s1i),
        (d0r - d1i, d0i + d1r),
    )


def expand_right(row_form):
    n = row_form.shape[-1] // 2
    r, i = row_form[:, :n], row_form[:, n:]
    return jnp.concatenate(
        [jnp.concatenate([r, i], 1), jnp.concatenate([-i, r], 1)], 0
    )


def lead_kernel(sc, pos, sig, w1, w2, w3, w4, *rest):
    outs, (ax_c, ax_s, by_c, by_s, table, c0, d, mm, w43, e21) = rest[:8], rest[8:]

    w = lax.broadcasted_iota(jnp.int32, (SIDE, 1), 0) - SIDE // 2
    xc, xs = sincos(w * pos[0:1, :])
    ax_c[...] = xc * (1.0 / 16.0)
    ax_s[...] = xs * (1.0 / 16.0)
    yc, ys = sincos(w * pos[1:2, :])
    by_c[...] = yc
    by_s[...] = ys

    row = lax.broadcasted_iota(jnp.int32, (K, K), 0)
    col = lax.broadcasted_iota(jnp.int32, (K, K), 1)
    kx, ky = row // 64, row // 16 % 4
    hx, hy = row // 4 % 4, row % 4
    source = (hx * 4 + kx) * 16 + hy * 4 + ky
    pick = jnp.where(source == col, 1.0, 0.0).astype(BF)

    def row_form(ref, r):
        return jnp.concatenate([ref[0, r, 0, 0], ref[0, r, 0, 1]], 1)

    upper = jnp.concatenate(
        [dot(pick, row_form(w4, r)).astype(BF) for r in range(2)], 0
    )
    for r3 in range(2):
        w43[pl.ds(r3 * 512, 512), :] = dot(upper, expand_right(row_form(w3, r3))).astype(BF)
    lower = jnp.concatenate([row_form(w2, r) for r in range(2)], 0)
    for r1 in range(2):
        both = dot(lower, expand_right(row_form(w1, r1))).astype(BF)
        for r2 in range(2):
            e21[r1 * 2 + r2] = expand_right(both[r2 * K : (r2 + 1) * K])

    first = sc[0] == 0
    own_z, own_x = sc[1], sc[2]

    def composite(z, _):
        rz = place(jnp.bitwise_and(z - own_z, 3))
        right = e21[z]
        for x in range(4):
            rx = place(jnp.bitwise_and(x - own_x, 3))
            slot = jnp.where(first, rz * 4 + rx, rx * 4 + rz)
            product = dot(w43[pl.ds(x * K, K), :], right).astype(BF)
            mm[:, slot] = product.reshape(16, 16, 512)
        return 0

    lax.fori_loop(0, 4, composite, 0)

    def leaf(m, _):
        start = pl.multiple_of(m * EB, EB)
        bc = by_c[:, pl.ds(start, EB)]
        bs = by_s[:, pl.ds(start, EB)]
        for wx in range(SIDE):
            ac = ax_c[wx : wx + 1, pl.ds(start, EB)]
            as_ = ax_s[wx : wx + 1, pl.ds(start, EB)]
            table[pl.ds(wx * 16, 16), 0:EB] = (ac * bc - as_ * bs).astype(BF)
            table[pl.ds(wx * 16, 16), EB : 2 * EB] = (as_ * bc + ac * bs).astype(BF)
        t = table[...]
        for h in range(NH):
            sr = sig[0, pl.ds(start, EB), h * HALF : (h + 1) * HALF]
            si = sig[1, pl.ds(start, EB), h * HALF : (h + 1) * HALF]
            right = jnp.concatenate(
                [jnp.concatenate([sr, si], 1), jnp.concatenate([si, -sr], 1)], 0
            )
            c0[h, m] = dot(t, right)
        return 0

    lax.fori_loop(0, BOXES, leaf, 0)

    def along_x(i, _):
        rows = pl.ds(pl.multiple_of(i * 16, 16), 16)
        for h in range(NH):
            for my in range(4):
                x = [
                    (c0[h, my * 4 + mx, rows, 0:HALF], c0[h, my * 4 + mx, rows, HALF:])
                    for mx in range(4)
                ]
                for kx_, (re, im) in enumerate(dft4(x)):
                    c0[h, my * 4 + kx_, rows, 0:HALF] = re
                    c0[h, my * 4 + kx_, rows, HALF:] = im
        return 0

    lax.fori_loop(0, 16, along_x, 0)

    def along_y(i, _):
        rows = pl.ds(pl.multiple_of(i * 16, 16), 16)
        low = pl.ds(pl.multiple_of(i * 16 + K, 16), 16)
        for h in range(NH):
            for kx_ in range(4):
                x = [
                    (c0[h, my * 4 + kx_, rows, 0:HALF], c0[h, my * 4 + kx_, rows, HALF:])
                    for my in range(4)
                ]
                for ky_, (re, im) in enumerate(dft4(x)):
                    re = (re * 0.25).astype(BF)
                    im = (im * 0.25).astype(BF)
                    cls = kx_ * 4 + ky_
                    d[h, cls, rows, 0:HALF] = re
                    d[h, cls, rows, HALF:] = im
                    d[h, cls, low, 0:HALF] = -im
                    d[h, cls, low, HALF:] = re
        return 0

    lax.fori_loop(0, 16, along_y, 0)

    def apply(cls, _):
        left = mm[cls].reshape(K, 2 * K)
        rows = pl.ds(pl.multiple_of(cls * 16, 16), 16)
        for h in range(NH):
            out = dot(left, d[h, cls]).astype(BF).reshape(4, 4, 16, 2 * HALF)
            for dp in range(4):
                outs[h * 4 + dp][:, rows, :] = out[dp]
        return 0

    lax.fori_loop(0, 16, apply, 0)


def lead(sc, positions, signal, weights):
    def w_spec(level):
        return pl.BlockSpec(
            (1, 2, 1, 2, K, K), lambda i, s: (level, 0, s[3 + level], 0, 0, 0)
        )

    whole = lambda shape: pl.BlockSpec(shape, lambda i, s: (0,) * len(shape))
    ne = positions.shape[1]
    return pl.pallas_call(
        lead_kernel,
        out_shape=[jax.ShapeDtypeStruct((4, K, 2 * HALF), BF)] * 8,
        grid_spec=pltpu.PrefetchScalarGridSpec(
            num_scalar_prefetch=1,
            grid=(1,),
            in_specs=[whole((2, ne)), whole(signal.shape)] + [w_spec(i) for i in range(4)],
            out_specs=[whole((4, K, 2 * HALF))] * 8,
            scratch_shapes=[pltpu.VMEM((SIDE, ne), F32)] * 4
            + [
                pltpu.VMEM((K, 2 * EB), BF),
                pltpu.VMEM((NH, BOXES, K, 2 * HALF), F32),
                pltpu.VMEM((NH, 16, 2 * K, 2 * HALF), BF),
                pltpu.VMEM((16, 16, 16, 2 * K), BF),
                pltpu.VMEM((4 * K, 2 * K), BF),
                pltpu.VMEM((4, 2 * K, 2 * K), BF),
            ],
        ),
        compiler_params=pltpu.CompilerParams(vmem_limit_bytes=56 << 20),
        cost_estimate=pl.CostEstimate(
            flops=8_000_000_000, transcendentals=0, bytes_accessed=12 << 20
        ),
        name="lead",
    )(sc, positions, signal, weights, weights, weights, weights)


def steer_kernel(pos, out, table):
    r = lax.broadcasted_iota(jnp.int32, (SIDE, 1), 0)
    n = pos.shape[-1]
    u, v = pos[0, 0:1, :], pos[1, 0:1, :]
    for kx in range(4):
        ac, as_ = sincos((r // 4 * 4 + kx - 8) * u)
        ac, as_ = ac * (1.0 / 16.0), as_ * (1.0 / 16.0)
        for ky in range(4):
            bc, bs = sincos((r % 4 * 4 + ky - 8) * v)
            rows = pl.ds((kx * 4 + ky) * 16, 16)
            table[rows, :] = ac * bc - as_ * bs
            table[pl.ds((kx * 4 + ky) * 16 + K, 16), :] = as_ * bc + ac * bs
    for i in range(n // 128):
        for j in range(2 * K // 128):
            block = table[pl.ds(j * 128, 128), pl.ds(i * 128, 128)]
            out[pl.ds(i * 128, 128), pl.ds(j * 128, 128)] = block.T.astype(BF)


def steer(directions):
    n = directions.shape[-1]
    return pl.pallas_call(
        steer_kernel,
        out_shape=jax.ShapeDtypeStruct((n, 2 * K), BF),
        scratch_shapes=[pltpu.VMEM((2 * K, n), F32)],
        cost_estimate=pl.CostEstimate(
            flops=1_000_000_000, transcendentals=0, bytes_accessed=1 << 20
        ),
        name="steer",
    )(directions)


def sum_split_kernel(a, b, c, d, *outs):
    for i, o in enumerate(outs):
        t = a[i].astype(F32) + b[i].astype(F32) + c[i].astype(F32) + d[i].astype(F32)
        o[...] = t.astype(BF)


def sum_split(a, b, c, d):
    return pl.pallas_call(
        sum_split_kernel,
        out_shape=[jax.ShapeDtypeStruct(a.shape[1:], BF)] * a.shape[0],
        name="sum_split",
    )(a, b, c, d)


def sum_four_kernel(a, b, c, d, o):
    t = a[...].astype(F32) + b[...].astype(F32) + c[...].astype(F32) + d[...].astype(F32)
    o[...] = t.astype(BF)


def sum_four(a, b, c, d):
    return pl.pallas_call(
        sum_four_kernel, out_shape=jax.ShapeDtypeStruct(a.shape, BF), name="sum_four"
    )(a, b, c, d)


def beam_kernel(blocks, table, z0, z1, z2, z3, *rest):
    out = rest[-1]
    for i, z in enumerate((z0, z1, z2, z3)):

        @pl.when(pl.program_id(0) == i)
        def _():
            b = dot(table[...], expand_right(z[...])).astype(BF)
            out[0, 0] = b[:, :HALF]
            out[1, 0] = b[:, HALF:]


def beams(blocks, table, parts, previous, shape):
    n = table.shape[0]
    whole = lambda shape: pl.BlockSpec(shape, lambda i, s: (0,) * len(shape))
    extra = [] if previous is None else [previous]
    return pl.pallas_call(
        beam_kernel,
        out_shape=jax.ShapeDtypeStruct(shape, BF),
        grid_spec=pltpu.PrefetchScalarGridSpec(
            num_scalar_prefetch=1,
            grid=(4,),
            in_specs=[whole(table.shape)]
            + [whole((K, 2 * HALF))] * 4
            + [pl.BlockSpec(memory_space=pl.ANY)] * len(extra),
            out_specs=pl.BlockSpec((2, 1, n, HALF), lambda i, s: (0, 0, 0, s[i])),
        ),
        input_output_aliases={} if previous is None else {6: 0},
        name="beams",
    )(blocks, table, *parts, *extra)


def ring(step, first):
    pairs = []
    for z in range(4):
        for x in range(4):
            along_z = ((z + step) % 4) * 4 + x
            along_x = z * 4 + (x + step) % 4
            core0, core1 = (along_z, along_x) if first else (along_x, along_z)
            pairs.append((z * 4 + x, core0))
            pairs.append((16 + z * 4 + x, 16 + core1))
    return pairs


def local(signal, positions, weights, directions):
    core = lax.axis_index("freq")
    z, x, y = lax.axis_index("z"), lax.axis_index("x"), lax.axis_index("dir")
    sc = jnp.stack([core, z, x, z // 2, z % 2, x // 2, x % 2]).astype(jnp.int32)
    pieces = lead(sc, positions, signal, weights)
    table = steer(directions)
    along = ("freq", "z", "x")
    cols = signal.shape[2] * 4
    shape = (2, 1, directions.shape[2], cols)
    result = None
    for h in range(NH):
        p2, p1, m1, own = pieces[4 * h : 4 * h + 4]
        r2 = lax.ppermute(p2, along, ring(2, True))
        r1 = lax.ppermute(p1, along, ring(1, True))
        rm = lax.ppermute(m1, along, ring(-1, True))
        s2, s1, sm, s0 = sum_split(own, r1, rm, r2)
        t2 = lax.ppermute(s2, along, ring(2, False))
        t1 = lax.ppermute(s1, along, ring(1, False))
        tm = lax.ppermute(sm, along, ring(-1, False))
        zz = sum_four(s0, t1, tm, t2)
        y2 = lax.ppermute(zz, "dir", [(i, (i + 2) % 4) for i in range(4)])
        y1 = lax.ppermute(zz, "dir", [(i, (i + 1) % 4) for i in range(4)])
        ym = lax.ppermute(zz, "dir", [(i, (i + 3) % 4) for i in range(4)])
        order = jnp.stack([y, (y + 3) % 4, (y + 1) % 4, (y + 2) % 4]) * NH + h
        result = beams(order.astype(jnp.int32), table, (zz, y1, ym, y2), result, shape)
    return result


def solution(mesh):
    split = Mesh(
        mesh.devices.reshape(2, 4, 4, 4), ("freq", "dir", "z", "x")
    )
    ap = ("z", "x")
    in_specs = (P(None, ap, ("freq", "dir")), P(None, ap), P(), P(None, ap, "dir"))
    out_specs = P(None, ap, "dir", "freq")
    return jax.shard_map(
        local, mesh=split, in_specs=in_specs, out_specs=out_specs, check_vma=False
    )
```

```python
import math

import jax
import jax.numpy as jnp
from jax import lax
from jax.experimental import pallas as pl
from jax.experimental.pallas import tpu as pltpu
from jax.sharding import Mesh, PartitionSpec as P

K = 256
EB = 256
SIDE = 16
BOXES = 16
COLS = 256
F32 = jnp.float32
BF = jnp.bfloat16


def sincos(phase):
    p = jnp.bitwise_and(phase, 255)
    q = jnp.right_shift(p + 32, 6)
    t = (p - jnp.left_shift(q, 6)).astype(F32) * (2.0 * math.pi / 256.0)
    u = t * t
    s0 = t * (1.0 + u * (-1.0 / 6 + u * (1.0 / 120 + u * (-1.0 / 5040 + u * (1.0 / 362880)))))
    c0 = 1.0 + u * (-0.5 + u * (1.0 / 24 + u * (-1.0 / 720 + u * (1.0 / 40320))))
    odd = jnp.bitwise_and(q, 1) == 1
    c = jnp.where(odd, s0, c0)
    s = jnp.where(odd, c0, s0)
    c = jnp.where(jnp.bitwise_and(q + 1, 2) == 2, -c, c)
    s = jnp.where(jnp.bitwise_and(q, 2) == 2, -s, s)
    return c, s


def dot(a, b):
    return jnp.dot(a, b, preferred_element_type=F32)


def place(offset):
    return jnp.where(offset == 0, 3, jnp.where(offset == 2, 0, jnp.where(offset == 1, 1, 2)))


def dft4(x):
    (a, b), (c, d), (e, f), (g, h) = x
    s0r, s0i, d0r, d0i = a + e, b + f, a - e, b - f
    s1r, s1i, d1r, d1i = c + g, d + h, c - g, d - h
    return (
        (s0r + s1r, s0i + s1i),
        (d0r + d1i, d0i - d1r),
        (s0r - s1r, s0i - s1i),
        (d0r - d1i, d0i + d1r),
    )


def expand_right(row_form):
    n = row_form.shape[-1] // 2
    r, i = row_form[:, :n], row_form[:, n:]
    return jnp.concatenate(
        [jnp.concatenate([r, i], 1), jnp.concatenate([-i, r], 1)], 0
    )


VMEM = pltpu.VMEM


def lead_kernel(pos, sig_hbm, w_hbm, *rest):
    outs, scratch = rest[:5], rest[5:]
    p2lo, p2hi, q1, qm, own = outs
    sig, w, ax_c, ax_s, by_c, by_s, t0, t1, c0, d, mm, w43, e21, wsem, ssem = scratch
    core, own_z, own_x = (lax.axis_index(n) for n in ("freq", "z", "x"))
    child = (own_z // 2, own_z % 2, own_x // 2, own_x % 2)

    w_copies = [
        pltpu.make_async_copy(w_hbm.at[i, :, child[i]], w.at[i], wsem.at[i])
        for i in range(4)
    ]
    for i in (3, 2, 1, 0):
        w_copies[i].start()
    quarter = sig.shape[1] // 4
    s_copies = [
        pltpu.make_async_copy(
            sig_hbm.at[:, pl.ds(i * quarter, quarter), :],
            sig.at[:, pl.ds(i * quarter, quarter), :],
            ssem.at[i],
        )
        for i in range(4)
    ]
    for c in s_copies:
        c.start()

    wave = lax.broadcasted_iota(jnp.int32, (SIDE, 1), 0) - SIDE // 2

    def factors(i, _):
        lanes = pl.ds(pl.multiple_of(i * 512, 512), 512)
        xc, xs = sincos(wave * pos[0:1, lanes])
        ax_c[:, lanes] = xc * (1.0 / 16.0)
        ax_s[:, lanes] = xs * (1.0 / 16.0)
        yc, ys = sincos(wave * pos[1:2, lanes])
        by_c[:, lanes] = yc
        by_s[:, lanes] = ys
        return 0

    lax.fori_loop(0, pos.shape[1] // 512, factors, 0)

    row = lax.broadcasted_iota(jnp.int32, (K, K), 0)
    col = lax.broadcasted_iota(jnp.int32, (K, K), 1)
    kx, ky = row // 64, row // 16 % 4
    hx, hy = row // 4 % 4, row % 4
    source = (hx * 4 + kx) * 16 + hy * 4 + ky
    pick = jnp.where(source == col, 1.0, 0.0).astype(BF)

    def row_form(level, r):
        return jnp.concatenate([w[level, r, 0], w[level, r, 1]], 1)

    w_copies[3].wait()
    upper = jnp.concatenate(
        [dot(pick, row_form(3, r)).astype(BF) for r in range(2)], 0
    )
    w_copies[2].wait()
    for r3 in range(2):
        w43[pl.ds(r3 * 512, 512), :] = dot(upper, expand_right(row_form(2, r3))).astype(BF)
    w_copies[1].wait()
    w_copies[0].wait()
    lower = jnp.concatenate([row_form(1, r) for r in range(2)], 0)
    for r1 in range(2):
        both = dot(lower, expand_right(row_form(0, r1))).astype(BF)
        for r2 in range(2):
            e21[r1 * 2 + r2] = expand_right(both[r2 * K : (r2 + 1) * K])

    first = core == 0

    def composite(z, _):
        rz = place(jnp.bitwise_and(z - own_z, 3))
        right = e21[z]
        for x in range(4):
            rx = place(jnp.bitwise_and(x - own_x, 3))
            slot = jnp.where(first, rz * 4 + rx, rx * 4 + rz)
            product = dot(w43[pl.ds(x * K, K), :], right).astype(BF)
            mm[:, slot] = product.reshape(16, 16, 512)
        return 0

    lax.fori_loop(0, 4, composite, 0)

    def build(table, m):
        start = pl.multiple_of(m * EB, EB)
        bc = by_c[:, pl.ds(start, EB)]
        bs = by_s[:, pl.ds(start, EB)]
        for wx in range(SIDE):
            ac = ax_c[wx : wx + 1, pl.ds(start, EB)]
            as_ = ax_s[wx : wx + 1, pl.ds(start, EB)]
            table[pl.ds(wx * 16, 16), 0:EB] = (ac * bc - as_ * bs).astype(BF)
            table[pl.ds(wx * 16, 16), EB : 2 * EB] = (as_ * bc + ac * bs).astype(BF)

    def multiply(table, m):
        start = pl.multiple_of(m * EB, EB)
        sr = sig[0, pl.ds(start, EB), :]
        si = sig[1, pl.ds(start, EB), :]
        right = jnp.concatenate(
            [jnp.concatenate([sr, si], 1), jnp.concatenate([si, -sr], 1)], 0
        )
        c0[m] = dot(table[...], right)

    build(t0, 0)
    for c in s_copies:
        c.wait()

    def leaf(i, _):
        m = i * 2
        build(t1, m + 1)
        multiply(t0, m)
        build(t0, jnp.minimum(m + 2, BOXES - 1))
        multiply(t1, m + 1)
        return 0

    lax.fori_loop(0, BOXES // 2, leaf, 0)

    def along_x(i, _):
        rows = pl.ds(pl.multiple_of(i * 8, 8), 8)
        for half in range(2):
            re_at, im_at = pl.ds(half * 128, 128), pl.ds(COLS + half * 128, 128)
            for my in range(4):
                x = [(c0[my * 4 + mx, rows, re_at], c0[my * 4 + mx, rows, im_at]) for mx in range(4)]
                for kx_, (re, im) in enumerate(dft4(x)):
                    c0[my * 4 + kx_, rows, re_at] = re
                    c0[my * 4 + kx_, rows, im_at] = im
        return 0

    lax.fori_loop(0, K // 8, along_x, 0)

    def along_y(i, _):
        rows = pl.ds(pl.multiple_of(i * 16, 16), 16)
        low = pl.ds(pl.multiple_of(i * 16 + K, 16), 16)
        for half in range(2):
            re_at, im_at = pl.ds(half * 128, 128), pl.ds(COLS + half * 128, 128)
            for kx_ in range(4):
                x = [(c0[my * 4 + kx_, rows, re_at], c0[my * 4 + kx_, rows, im_at]) for my in range(4)]
                for ky_, (re, im) in enumerate(dft4(x)):
                    re = (re * 0.25).astype(BF)
                    im = (im * 0.25).astype(BF)
                    cls = kx_ * 4 + ky_
                    d[cls, rows, re_at] = re
                    d[cls, rows, im_at] = im
                    d[cls, low, re_at] = -im
                    d[cls, low, im_at] = re
        return 0

    lax.fori_loop(0, K // 16, along_y, 0)

    def apply(cls, _):
        left = mm[cls].reshape(K, 2 * K)
        rows = pl.ds(pl.multiple_of(cls * 16, 16), 16)
        out = dot(left, d[cls]).astype(BF).reshape(4, 4, 16, 2 * COLS)
        p2lo[:, rows, :] = out[0, 0:2]
        p2hi[:, rows, :] = out[0, 2:4]
        q1[:, rows, :] = out[1]
        qm[:, rows, :] = out[2]
        own[:, rows, :] = out[3]
        return 0

    lax.fori_loop(0, 16, apply, 0)


def vm(n):
    return [pl.BlockSpec(memory_space=VMEM)] * n


def shaped(*dims, dtype=BF):
    return jax.ShapeDtypeStruct(dims, dtype)


def lead(positions, signal, weights):
    ne = positions.shape[1]
    hbm = pl.BlockSpec(memory_space=pl.ANY)
    return pl.pallas_call(
        lead_kernel,
        out_shape=[shaped(n, K, 2 * COLS) for n in (2, 2, 4, 4, 4)],
        in_specs=vm(1) + [hbm, hbm],
        out_specs=vm(5),
        scratch_shapes=[VMEM(signal.shape, BF), VMEM((4, 2, 2, K, K), BF)]
        + [VMEM((SIDE, ne), F32)] * 4
        + [VMEM((K, 2 * EB), BF)] * 2
        + [
            VMEM((BOXES, K, 2 * COLS), F32),
            VMEM((16, 2 * K, 2 * COLS), BF),
            VMEM((16, 16, 16, 2 * K), BF),
            VMEM((4 * K, 2 * K), BF),
            VMEM((4, 2 * K, 2 * K), BF),
            pltpu.SemaphoreType.DMA((4,)),
            pltpu.SemaphoreType.DMA((4,)),
        ],
        compiler_params=pltpu.CompilerParams(vmem_limit_bytes=44 << 20),
        cost_estimate=pl.CostEstimate(
            flops=8_000_000_000, transcendentals=0, bytes_accessed=12 << 20
        ),
        name="lead",
    )(positions, signal, weights)


def steer_kernel(pos, out, table):
    r = lax.broadcasted_iota(jnp.int32, (SIDE, 1), 0)
    n = pos.shape[-1]
    u, v = pos[0, 0:1, :], pos[1, 0:1, :]
    for kx in range(4):
        ac, as_ = sincos((r // 4 * 4 + kx - 8) * u)
        ac, as_ = ac * (1.0 / 16.0), as_ * (1.0 / 16.0)
        for ky in range(4):
            bc, bs = sincos((r % 4 * 4 + ky - 8) * v)
            rows = pl.ds((kx * 4 + ky) * 16, 16)
            table[rows, :] = ac * bc - as_ * bs
            table[pl.ds((kx * 4 + ky) * 16 + K, 16), :] = as_ * bc + ac * bs
    for i in range(n // 128):
        for j in range(2 * K // 128):
            block = table[pl.ds(j * 128, 128), pl.ds(i * 128, 128)]
            out[pl.ds(i * 128, 128), pl.ds(j * 128, 128)] = block.T.astype(BF)


def steer(directions):
    n = directions.shape[-1]
    return pl.pallas_call(
        steer_kernel,
        out_shape=shaped(n, 2 * K),
        in_specs=vm(1),
        out_specs=vm(1)[0],
        scratch_shapes=[VMEM((2 * K, n), F32)],
        cost_estimate=pl.CostEstimate(
            flops=1_500_000_000, transcendentals=0, bytes_accessed=1 << 20
        ),
        compiler_params=pltpu.CompilerParams(vmem_limit_bytes=16 << 20),
        name="steer",
    )(directions)


def added(*terms):
    total = terms[0].astype(F32)
    for t in terms[1:]:
        total = total + t.astype(F32)
    return total


def call(kernel, shapes, name, *args):
    return pl.pallas_call(
        kernel,
        out_shape=shapes,
        in_specs=vm(len(args)),
        out_specs=vm(len(shapes)),
        compiler_params=pltpu.CompilerParams(vmem_limit_bytes=24 << 20),
        name=name,
    )(*args)


def merge_kernel(q1, qm, rlo, rhi, f1a, fma, f1b, fmb):
    f1a[...] = added(q1[0], rlo[0]).astype(BF)
    fma[...] = qm[0]
    f1b[0] = added(q1[1], rlo[1]).astype(BF)
    f1b[1] = q1[2]
    f1b[2] = q1[3]
    fmb[0] = qm[1]
    fmb[1] = added(qm[2], rhi[0]).astype(BF)
    fmb[2] = added(qm[3], rhi[1]).astype(BF)


def sum_far_kernel(own, g1a, gma, lo, hi):
    s = added(own[0], g1a[...], gma[...]).astype(BF)
    lo[...] = s[: K // 2]
    hi[...] = s[K // 2 :]


def sum_near_kernel(own, g1b, gmb, tlo, thi, u1, um, s0):
    h = K // 2
    one = added(own[1], g1b[0], gmb[0])
    u1[0:h] = (one[:h] + tlo[...].astype(F32)).astype(BF)
    u1[h:] = one[h:].astype(BF)
    other = added(own[2], g1b[1], gmb[1])
    um[0:h] = other[:h].astype(BF)
    um[h:] = (other[h:] + thi[...].astype(F32)).astype(BF)
    s0[...] = added(own[3], g1b[2], gmb[2])


def total_kernel(s0, v1, vm_, z):
    z[...] = added(s0[...], v1[...], vm_[...]).astype(BF)


def beam_kernel(offsets, table, *rest):
    parts = rest[: len(offsets)]
    out, buf, sem = rest[-3:]
    y = lax.axis_index("dir")
    n = table.shape[0] // 2
    copies = []
    for i, offset in enumerate(offsets):
        right = expand_right(parts[i][...])
        column = pl.multiple_of(jnp.bitwise_and(y + offset, 3) * COLS, COLS)
        for r in range(2):
            slot = len(copies) % 2
            if len(copies) >= 2:
                copies[-2].wait()
            b = dot(table[pl.ds(r * n, n), :], right).astype(BF)
            buf[slot, 0] = b[:, :COLS]
            buf[slot, 1] = b[:, COLS:]
            copies.append(
                pltpu.make_async_copy(
                    buf.at[slot],
                    out.at[:, 0, pl.ds(r * n, n), pl.ds(column, COLS)],
                    sem.at[slot],
                )
            )
            copies[-1].start()
    for c in copies[-2:]:
        c.wait()


def beams(offsets, table, parts, previous, shape):
    n = table.shape[0]
    hbm = pl.BlockSpec(memory_space=pl.ANY)
    extra = [] if previous is None else [previous]
    return pl.pallas_call(
        lambda *refs: beam_kernel(offsets, *refs),
        out_shape=jax.ShapeDtypeStruct(shape, BF),
        in_specs=vm(1 + len(parts)) + [hbm] * len(extra),
        out_specs=hbm,
        scratch_shapes=[
            VMEM((2, 2, n // 2, COLS), BF),
            pltpu.SemaphoreType.DMA((2,)),
        ],
        input_output_aliases={} if previous is None else {1 + len(parts): 0},
        cost_estimate=pl.CostEstimate(
            flops=2_000_000_000, transcendentals=0, bytes_accessed=1 << 20
        ),
        compiler_params=pltpu.CompilerParams(vmem_limit_bytes=24 << 20),
        name="beams",
    )(table, *parts, *extra)


def ring(step, first):
    pairs = []
    for z in range(4):
        for x in range(4):
            along_z = ((z + step) % 4) * 4 + x
            along_x = z * 4 + (x + step) % 4
            core0, core1 = (along_z, along_x) if first else (along_x, along_z)
            pairs.append((z * 4 + x, core0))
            pairs.append((16 + z * 4 + x, 16 + core1))
    return pairs


def local(signal, positions, weights, directions):
    along = ("freq", "z", "x")

    def major(a, step):
        return lax.ppermute(a, along, ring(step, True))

    def minor(a, step):
        return lax.ppermute(a, along, ring(step, False))

    def across(a, step):
        return lax.ppermute(a, "dir", [(i, (i + step) % 4) for i in range(4)])

    p2lo, p2hi, q1, qm, own = lead(positions, signal, weights)
    table = steer(directions)
    block = (K, 2 * COLS)
    rlo, rhi = major(p2lo, 1), major(p2hi, -1)
    f1a, fma, f1b, fmb = call(
        merge_kernel,
        [shaped(*block), shaped(*block), shaped(3, *block), shaped(3, *block)],
        "merge", q1, qm, rlo, rhi,
    )
    g1a, gma = major(f1a, 1), major(fma, -1)
    g1b, gmb = major(f1b, 1), major(fmb, -1)
    half = shaped(K // 2, 2 * COLS)
    lo, hi = call(sum_far_kernel, [half, half], "sum_far", own, g1a, gma)
    tlo, thi = minor(lo, 1), minor(hi, -1)
    u1, um, s0 = call(
        sum_near_kernel,
        [shaped(*block), shaped(*block), shaped(*block, dtype=F32)],
        "sum_near", own, g1b, gmb, tlo, thi,
    )
    v1, v_m = minor(u1, 1), minor(um, -1)
    (zz,) = call(total_kernel, [shaped(*block)], "total", s0, v1, v_m)
    y2, y1, ym = across(zz, 2), across(zz, 1), across(zz, -1)
    shape = (2, 1, directions.shape[2], signal.shape[2] * 4)
    result = beams((0,), table, (zz,), None, shape)
    return beams((3, 1, 2), table, (y1, ym, y2), result, shape)


def solution(mesh):
    split = Mesh(mesh.devices.reshape(2, 4, 4, 4), ("freq", "dir", "z", "x"))
    ap = ("z", "x")
    in_specs = (P(None, ap, ("freq", "dir")), P(None, ap), P(), P(None, ap, "dir"))
    out_specs = P(None, ap, "dir", "freq")
    return jax.shard_map(
        local, mesh=split, in_specs=in_specs, out_specs=out_specs, check_vma=False
    )
```

```python
import math

import jax
import jax.numpy as jnp
from jax import lax
from jax.experimental import pallas as pl
from jax.experimental.pallas import tpu as pltpu
from jax.sharding import Mesh, PartitionSpec as P


K = 256
EB = 256
SIDE = 16
BOXES = 16
COLS = 256
F32 = jnp.float32
BF = jnp.bfloat16


def sincos(phase):
    p = jnp.bitwise_and(phase, 255)
    q = jnp.right_shift(p + 32, 6)
    t = (p - jnp.left_shift(q, 6)).astype(F32) * (2.0 * math.pi / 256.0)
    u = t * t
    s0 = t * (1.0 + u * (-1.0 / 6 + u * (1.0 / 120 + u * (-1.0 / 5040 + u * (1.0 / 362880)))))
    c0 = 1.0 + u * (-0.5 + u * (1.0 / 24 + u * (-1.0 / 720 + u * (1.0 / 40320))))
    odd = jnp.bitwise_and(q, 1) == 1
    c = jnp.where(odd, s0, c0)
    s = jnp.where(odd, c0, s0)
    c = jnp.where(jnp.bitwise_and(q + 1, 2) == 2, -c, c)
    s = jnp.where(jnp.bitwise_and(q, 2) == 2, -s, s)
    return c, s


def dot(a, b):
    return jnp.dot(a, b, preferred_element_type=F32)


def place(offset):
    return jnp.where(offset == 0, 3, jnp.where(offset == 2, 0, jnp.where(offset == 1, 1, 2)))


def dft4(x):
    (a, b), (c, d), (e, f), (g, h) = x
    s0r, s0i, d0r, d0i = a + e, b + f, a - e, b - f
    s1r, s1i, d1r, d1i = c + g, d + h, c - g, d - h
    return (
        (s0r + s1r, s0i + s1i),
        (d0r + d1i, d0i - d1r),
        (s0r - s1r, s0i - s1i),
        (d0r - d1i, d0i + d1r),
    )


def expand_right(row_form):
    n = row_form.shape[-1] // 2
    r, i = row_form[:, :n], row_form[:, n:]
    return jnp.concatenate(
        [jnp.concatenate([r, i], 1), jnp.concatenate([-i, r], 1)], 0
    )


VMEM = pltpu.VMEM


def lead_kernel(pos_hbm, sig_hbm, w_hbm, *rest):
    outs, scratch = rest[:7], rest[7:]
    p2hi, p2lo, q1u, q1w, qmw, qmu, own = outs
    pos, sig, w, ax_c, ax_s, by_c, by_s, t0, t1, c0, d, mm, w43, e21, wsem, ssem = scratch
    core, own_z, own_x = (lax.axis_index(n) for n in ("freq", "z", "x"))
    child = (own_z // 2, own_z % 2, own_x // 2, own_x % 2)

    pos_copy = pltpu.make_async_copy(pos_hbm, pos, wsem.at[4])
    pos_copy.start()
    w_copies = [
        pltpu.make_async_copy(w_hbm.at[i, :, child[i]], w.at[i], wsem.at[i])
        for i in range(4)
    ]
    for i in (3, 2, 1, 0):
        w_copies[i].start()
    quarter = sig.shape[1] // 4
    s_copies = [
        pltpu.make_async_copy(
            sig_hbm.at[:, pl.ds(i * quarter, quarter), :],
            sig.at[:, pl.ds(i * quarter, quarter), :],
            ssem.at[i],
        )
        for i in range(4)
    ]
    for c in s_copies:
        c.start()

    pos_copy.wait()
    wave = lax.broadcasted_iota(jnp.int32, (SIDE, 1), 0) - SIDE // 2

    def factors(i, _):
        lanes = pl.ds(pl.multiple_of(i * 512, 512), 512)
        xc, xs = sincos(wave * pos[0:1, lanes])
        ax_c[:, lanes] = xc * (1.0 / 16.0)
        ax_s[:, lanes] = xs * (1.0 / 16.0)
        yc, ys = sincos(wave * pos[1:2, lanes])
        by_c[:, lanes] = yc
        by_s[:, lanes] = ys
        return 0

    lax.fori_loop(0, pos.shape[1] // 512, factors, 0)

    row = lax.broadcasted_iota(jnp.int32, (K, K), 0)
    col = lax.broadcasted_iota(jnp.int32, (K, K), 1)
    kx, ky = row // 64, row // 16 % 4
    hx, hy = row // 4 % 4, row % 4
    source = (hx * 4 + kx) * 16 + hy * 4 + ky
    pick = jnp.where(source == col, 1.0, 0.0).astype(BF)

    def row_form(level, r):
        return jnp.concatenate([w[level, r, 0], w[level, r, 1]], 1)

    w_copies[3].wait()
    upper = jnp.concatenate(
        [dot(pick, row_form(3, r)).astype(BF) for r in range(2)], 0
    )
    w_copies[2].wait()
    for r3 in range(2):
        w43[pl.ds(r3 * 512, 512), :] = dot(upper, expand_right(row_form(2, r3))).astype(BF)
    w_copies[1].wait()
    w_copies[0].wait()
    lower = jnp.concatenate([row_form(1, r) for r in range(2)], 0)
    for r1 in range(2):
        both = dot(lower, expand_right(row_form(0, r1))).astype(BF)
        for r2 in range(2):
            e21[r1 * 2 + r2] = expand_right(both[r2 * K : (r2 + 1) * K])

    first = core == 0

    def composite(z, _):
        rz = place(jnp.bitwise_and(z - own_z, 3))
        right = e21[z]
        for x in range(4):
            rx = place(jnp.bitwise_and(x - own_x, 3))
            slot = jnp.where(first, rz * 4 + rx, rx * 4 + rz)
            product = dot(w43[pl.ds(x * K, K), :], right).astype(BF)
            mm[:, slot] = product.reshape(16, 16, 512)
        return 0

    lax.fori_loop(0, 4, composite, 0)

    def build(table, m):
        start = pl.multiple_of(m * EB, EB)
        bc = by_c[:, pl.ds(start, EB)]
        bs = by_s[:, pl.ds(start, EB)]
        for wx in range(SIDE):
            ac = ax_c[wx : wx + 1, pl.ds(start, EB)]
            as_ = ax_s[wx : wx + 1, pl.ds(start, EB)]
            table[pl.ds(wx * 16, 16), 0:EB] = (ac * bc - as_ * bs).astype(BF)
            table[pl.ds(wx * 16, 16), EB : 2 * EB] = (as_ * bc + ac * bs).astype(BF)

    def multiply(table, m):
        start = pl.multiple_of(m * EB, EB)
        sr = sig[0, pl.ds(start, EB), :]
        si = sig[1, pl.ds(start, EB), :]
        right = jnp.concatenate(
            [jnp.concatenate([sr, si], 1), jnp.concatenate([si, -sr], 1)], 0
        )
        c0[m] = dot(table[...], right)

    build(t0, 0)
    for c in s_copies:
        c.wait()

    def leaf(i, _):
        m = i * 2
        build(t1, m + 1)
        multiply(t0, m)
        build(t0, jnp.minimum(m + 2, BOXES - 1))
        multiply(t1, m + 1)
        return 0

    lax.fori_loop(0, BOXES // 2, leaf, 0)

    def along_x(i, _):
        rows = pl.ds(pl.multiple_of(i * 8, 8), 8)
        for half in range(2):
            re_at, im_at = pl.ds(half * 128, 128), pl.ds(COLS + half * 128, 128)
            for my in range(4):
                x = [(c0[my * 4 + mx, rows, re_at], c0[my * 4 + mx, rows, im_at]) for mx in range(4)]
                for kx_, (re, im) in enumerate(dft4(x)):
                    c0[my * 4 + kx_, rows, re_at] = re
                    c0[my * 4 + kx_, rows, im_at] = im
        return 0

    lax.fori_loop(0, K // 8, along_x, 0)

    def along_y(i, _):
        rows = pl.ds(pl.multiple_of(i * 16, 16), 16)
        low = pl.ds(pl.multiple_of(i * 16 + K, 16), 16)
        for half in range(2):
            re_at, im_at = pl.ds(half * 128, 128), pl.ds(COLS + half * 128, 128)
            for kx_ in range(4):
                x = [(c0[my * 4 + kx_, rows, re_at], c0[my * 4 + kx_, rows, im_at]) for my in range(4)]
                for ky_, (re, im) in enumerate(dft4(x)):
                    re = (re * 0.25).astype(BF)
                    im = (im * 0.25).astype(BF)
                    cls = kx_ * 4 + ky_
                    d[cls, rows, re_at] = re
                    d[cls, rows, im_at] = im
                    d[cls, low, re_at] = -im
                    d[cls, low, im_at] = re
        return 0

    lax.fori_loop(0, K // 16, along_y, 0)

    def apply(cls, _):
        left = mm[cls].reshape(K, 2 * K)
        rows = pl.ds(pl.multiple_of(cls * 16, 16), 16)
        out = dot(left, d[cls]).astype(BF).reshape(4, 4, 16, 2 * COLS)
        p2hi[:, rows, :] = out[0, 0:2]
        p2lo[:, rows, :] = out[0, 2:4]
        q1u[:, rows, :] = out[1, 0:2]
        q1w[:, rows, :] = out[1, 2:4]
        qmw[:, rows, :] = out[2, 0:2]
        qmu[:, rows, :] = out[2, 2:4]
        own[:, rows, :] = out[3]
        return 0

    lax.fori_loop(0, 16, apply, 0)


def vm(n):
    return [pl.BlockSpec(memory_space=VMEM)] * n


def shaped(*dims, dtype=BF):
    return jax.ShapeDtypeStruct(dims, dtype)


def lead(positions, signal, weights):
    ne = positions.shape[1]
    hbm = pl.BlockSpec(memory_space=pltpu.HBM)
    return pl.pallas_call(
        lead_kernel,
        out_shape=[shaped(n, K, 2 * COLS) for n in (2, 2, 2, 2, 2, 2, 4)],
        in_specs=[hbm] * 3,
        out_specs=vm(7),
        scratch_shapes=[VMEM(positions.shape, jnp.int32), VMEM(signal.shape, BF), VMEM((4, 2, 2, K, K), BF)]
        + [VMEM((SIDE, ne), F32)] * 4
        + [VMEM((K, 2 * EB), BF)] * 2
        + [
            VMEM((BOXES, K, 2 * COLS), F32),
            VMEM((16, 2 * K, 2 * COLS), BF),
            VMEM((16, 16, 16, 2 * K), BF),
            VMEM((4 * K, 2 * K), BF),
            VMEM((4, 2 * K, 2 * K), BF),
            pltpu.SemaphoreType.DMA((5,)),
            pltpu.SemaphoreType.DMA((4,)),
        ],
        compiler_params=pltpu.CompilerParams(vmem_limit_bytes=48 << 20),
        cost_estimate=pl.CostEstimate(
            flops=8_000_000_000, transcendentals=0, bytes_accessed=12 << 20
        ),
        name="lead",
    )(positions, signal, weights)


def steer_kernel(pos, out, table):
    r = lax.broadcasted_iota(jnp.int32, (SIDE, 1), 0)
    n = pos.shape[-1]
    u, v = pos[0, 0:1, :], pos[1, 0:1, :]
    for kx in range(4):
        ac, as_ = sincos((r // 4 * 4 + kx - 8) * u)
        ac, as_ = ac * (1.0 / 16.0), as_ * (1.0 / 16.0)
        for ky in range(4):
            bc, bs = sincos((r % 4 * 4 + ky - 8) * v)
            rows = pl.ds((kx * 4 + ky) * 16, 16)
            table[rows, :] = ac * bc - as_ * bs
            table[pl.ds((kx * 4 + ky) * 16 + K, 16), :] = as_ * bc + ac * bs
    for i in range(n // 128):
        for j in range(2 * K // 128):
            block = table[pl.ds(j * 128, 128), pl.ds(i * 128, 128)]
            out[pl.ds(i * 128, 128), pl.ds(j * 128, 128)] = block.T.astype(BF)


def steer(directions):
    n = directions.shape[-1]
    return pl.pallas_call(
        steer_kernel,
        out_shape=shaped(n, 2 * K),
        in_specs=vm(1),
        out_specs=vm(1)[0],
        scratch_shapes=[VMEM((2 * K, n), F32)],
        cost_estimate=pl.CostEstimate(
            flops=1_500_000_000, transcendentals=0, bytes_accessed=1 << 20
        ),
        compiler_params=pltpu.CompilerParams(vmem_limit_bytes=16 << 20),
        name="steer",
    )(directions)


def added(*terms):
    total = terms[0].astype(F32)
    for t in terms[1:]:
        total = total + t.astype(F32)
    return total


def call(kernel, shapes, *args):
    return pl.pallas_call(
        kernel,
        out_shape=shapes,
        in_specs=vm(len(args)),
        out_specs=vm(len(shapes)),
        compiler_params=pltpu.CompilerParams(vmem_limit_bytes=24 << 20),
    )(*args)


def merge_kernel(mine, received, *outs):
    if len(outs) == 1:
        outs[0][...] = added(mine[...], received[...]).astype(BF)
    else:
        for i, o in enumerate(outs):
            o[...] = added(mine[i], received[i]).astype(BF)


def sum_far_kernel(own, g1, gm, lo, hi):
    s = added(own[0], g1[0], gm[...]).astype(BF)
    lo[...] = s[: K // 2]
    hi[...] = s[K // 2 :]


def sum_near_kernel(own, g1u, gmb, g1w, gmu, tlo, thi, u1, um, s0):
    h = K // 2
    one = added(own[1], g1u[1], gmb[...])
    u1[0:h] = (one[:h] + tlo[...].astype(F32)).astype(BF)
    u1[h:] = one[h:].astype(BF)
    other = added(own[2], g1w[0], gmu[0])
    um[0:h] = other[:h].astype(BF)
    um[h:] = (other[h:] + thi[...].astype(F32)).astype(BF)
    s0[...] = added(own[3], g1w[1], gmu[1])


def total_kernel(s0, v1, vm_, z):
    z[...] = added(s0[...], v1[...], vm_[...]).astype(BF)


def beam_kernel(offsets, table, *rest):
    parts = rest[: len(offsets)]
    out, buf, sem = rest[-3:]
    y = lax.axis_index("dir")
    n = table.shape[0] // 2
    copies = []
    for i, offset in enumerate(offsets):
        right = expand_right(parts[i][...])
        column = pl.multiple_of(jnp.bitwise_and(y + offset, 3) * COLS, COLS)
        for r in range(2):
            slot = len(copies) % 2
            if len(copies) >= 2:
                copies[-2].wait()
            b = dot(table[pl.ds(r * n, n), :], right).astype(BF)
            buf[slot, 0] = b[:, :COLS]
            buf[slot, 1] = b[:, COLS:]
            copies.append(
                pltpu.make_async_copy(
                    buf.at[slot],
                    out.at[:, 0, pl.ds(r * n, n), pl.ds(column, COLS)],
                    sem.at[slot],
                )
            )
            copies[-1].start()
    for c in copies[-2:]:
        c.wait()


def beams(offsets, table, parts, previous, shape):
    n = table.shape[0]
    hbm = pl.BlockSpec(memory_space=pltpu.HBM)
    extra = [] if previous is None else [previous]
    return pl.pallas_call(
        lambda *refs: beam_kernel(offsets, *refs),
        out_shape=jax.ShapeDtypeStruct(shape, BF),
        in_specs=vm(1 + len(parts)) + [hbm] * len(extra),
        out_specs=hbm,
        scratch_shapes=[
            VMEM((2, 2, n // 2, COLS), BF),
            pltpu.SemaphoreType.DMA((2,)),
        ],
        input_output_aliases={} if previous is None else {1 + len(parts): 0},
        cost_estimate=pl.CostEstimate(
            flops=2_000_000_000, transcendentals=0, bytes_accessed=1 << 20
        ),
        compiler_params=pltpu.CompilerParams(vmem_limit_bytes=24 << 20),
        name="beams",
    )(table, *parts, *extra)


def ring(step, first):
    pairs = []
    for z in range(4):
        for x in range(4):
            along_z = ((z + step) % 4) * 4 + x
            along_x = z * 4 + (x + step) % 4
            core0, core1 = (along_z, along_x) if first else (along_x, along_z)
            pairs.append((z * 4 + x, core0))
            pairs.append((16 + z * 4 + x, 16 + core1))
    return pairs


def local(signal, positions, weights, directions):
    along = ("freq", "z", "x")

    def major(a, step):
        return lax.ppermute(a, along, ring(step, True))

    def minor(a, step):
        return lax.ppermute(a, along, ring(step, False))

    def across(a, step):
        return lax.ppermute(a, "dir", [(i, (i + step) % 4) for i in range(4)])

    def compute():
        p2hi, p2lo, q1u, q1w, qmw, qmu, own = lead(positions, signal, weights)
        table = steer(directions)
        block = shaped(K, 2 * COLS)
        rhi, rlo = major(p2hi, -1), major(p2lo, 1)
        gmu, g1u = major(qmu, -1), major(q1u, 1)
        wma, wmb = call(merge_kernel, [block, block], qmw, rhi)
        (w1,) = call(merge_kernel, [shaped(2, K, 2 * COLS)], q1w, rlo)
        gma, g1w, gmb = major(wma, -1), major(w1, 1), major(wmb, -1)
        half = shaped(K // 2, 2 * COLS)
        lo, hi = call(sum_far_kernel, [half, half], own, g1u, gma)
        tlo, thi = minor(lo, 1), minor(hi, -1)
        u1, um, s0 = call(
            sum_near_kernel,
            [block, block, shaped(K, 2 * COLS, dtype=F32)],
            own, g1u, gmb, g1w, gmu, tlo, thi,
        )
        v1, v_m = minor(u1, 1), minor(um, -1)
        (zz,) = call(total_kernel, [block], s0, v1, v_m)
        y1, ym, y2 = across(zz, 1), across(zz, -1), across(zz, 2)
        shape = (2, 1, directions.shape[2], signal.shape[2] * 4)
        result = beams((0,), table, (zz,), None, shape)
        result = beams((3, 1), table, (y1, ym), result, shape)
        return beams((2,), table, (y2,), result, shape)

    return compute()


def solution(mesh):
    split = Mesh(mesh.devices.reshape(2, 4, 4, 4), ("freq", "dir", "z", "x"))
    ap = ("z", "x")
    in_specs = (P(None, ap, ("freq", "dir")), P(None, ap), P(), P(None, ap, "dir"))
    out_specs = P(None, ap, "dir", "freq")
    return jax.shard_map(
        local, mesh=split, in_specs=in_specs, out_specs=out_specs, check_vma=False
    )
```

```python
import math

import jax
import jax.numpy as jnp
from jax import lax
from jax.experimental import pallas as pl
from jax.experimental.pallas import tpu as pltpu
from jax.sharding import Mesh, PartitionSpec as P


K = 256
EB = 256
SIDE = 16
BOXES = 16
COLS = 256
F32 = jnp.float32
BF = jnp.bfloat16


def sincos(phase):
    p = jnp.bitwise_and(phase, 255)
    q = jnp.right_shift(p + 32, 6)
    t = (p - jnp.left_shift(q, 6)).astype(F32) * (2.0 * math.pi / 256.0)
    u = t * t
    s0 = t * (1.0 + u * (-1.0 / 6 + u * (1.0 / 120 + u * (-1.0 / 5040 + u * (1.0 / 362880)))))
    c0 = 1.0 + u * (-0.5 + u * (1.0 / 24 + u * (-1.0 / 720 + u * (1.0 / 40320))))
    odd = jnp.bitwise_and(q, 1) == 1
    c = jnp.where(odd, s0, c0)
    s = jnp.where(odd, c0, s0)
    c = jnp.where(jnp.bitwise_and(q + 1, 2) == 2, -c, c)
    s = jnp.where(jnp.bitwise_and(q, 2) == 2, -s, s)
    return c, s


def dot(a, b):
    return jnp.dot(a, b, preferred_element_type=F32)


def place(offset):
    return jnp.where(offset == 0, 3, jnp.where(offset == 2, 0, jnp.where(offset == 1, 1, 2)))


def dft4(x):
    (a, b), (c, d), (e, f), (g, h) = x
    s0r, s0i, d0r, d0i = a + e, b + f, a - e, b - f
    s1r, s1i, d1r, d1i = c + g, d + h, c - g, d - h
    return (
        (s0r + s1r, s0i + s1i),
        (d0r + d1i, d0i - d1r),
        (s0r - s1r, s0i - s1i),
        (d0r - d1i, d0i + d1r),
    )


def expand_right(row_form):
    n = row_form.shape[-1] // 2
    r, i = row_form[:, :n], row_form[:, n:]
    return jnp.concatenate(
        [jnp.concatenate([r, i], 1), jnp.concatenate([-i, r], 1)], 0
    )


VMEM = pltpu.VMEM


def lead_kernel(pos_hbm, sig_hbm, w_hbm, *rest):
    outs, scratch = rest[:7], rest[7:]
    p2hi, p2lo, q1u, q1w, qmw, qmu, own = outs
    pos, sig, w, ax_c, ax_s, by_c, by_s, t0, t1, c0, d, mm, w43, e21, wsem, ssem = scratch
    core, own_z, own_x = (lax.axis_index(n) for n in ("freq", "z", "x"))
    child = (own_z // 2, own_z % 2, own_x // 2, own_x % 2)

    pos_copy = pltpu.make_async_copy(pos_hbm, pos, wsem.at[4])
    pos_copy.start()
    w_copies = [
        pltpu.make_async_copy(w_hbm.at[i, :, child[i]], w.at[i], wsem.at[i])
        for i in range(4)
    ]
    for i in (3, 2, 1, 0):
        w_copies[i].start()
    quarter = sig.shape[1] // 4
    s_copies = [
        pltpu.make_async_copy(
            sig_hbm.at[:, pl.ds(i * quarter, quarter), :],
            sig.at[:, pl.ds(i * quarter, quarter), :],
            ssem.at[i],
        )
        for i in range(4)
    ]
    for c in s_copies:
        c.start()

    pos_copy.wait()
    wave = lax.broadcasted_iota(jnp.int32, (SIDE, 1), 0) - SIDE // 2

    def factors(i, _):
        lanes = pl.ds(pl.multiple_of(i * 512, 512), 512)
        xc, xs = sincos(wave * pos[0:1, lanes])
        ax_c[:, lanes] = xc * (1.0 / 16.0)
        ax_s[:, lanes] = xs * (1.0 / 16.0)
        yc, ys = sincos(wave * pos[1:2, lanes])
        by_c[:, lanes] = yc
        by_s[:, lanes] = ys
        return 0

    lax.fori_loop(0, pos.shape[1] // 512, factors, 0)

    row = lax.broadcasted_iota(jnp.int32, (K, K), 0)
    col = lax.broadcasted_iota(jnp.int32, (K, K), 1)
    kx, ky = row // 64, row // 16 % 4
    hx, hy = row // 4 % 4, row % 4
    source = (hx * 4 + kx) * 16 + hy * 4 + ky
    pick = jnp.where(source == col, 1.0, 0.0).astype(BF)

    def row_form(level, r):
        return jnp.concatenate([w[level, r, 0], w[level, r, 1]], 1)

    w_copies[3].wait()
    upper = jnp.concatenate(
        [dot(pick, row_form(3, r)).astype(BF) for r in range(2)], 0
    )
    w_copies[2].wait()
    for r3 in range(2):
        w43[pl.ds(r3 * 512, 512), :] = dot(upper, expand_right(row_form(2, r3))).astype(BF)
    w_copies[1].wait()
    w_copies[0].wait()
    lower = jnp.concatenate([row_form(1, r) for r in range(2)], 0)
    for r1 in range(2):
        both = dot(lower, expand_right(row_form(0, r1))).astype(BF)
        for r2 in range(2):
            e21[r1 * 2 + r2] = expand_right(both[r2 * K : (r2 + 1) * K])

    first = core == 0

    for z in range(4):
        rz = place(jnp.bitwise_and(z - own_z, 3))
        right = e21[z]
        for x in range(4):
            rx = place(jnp.bitwise_and(x - own_x, 3))
            slot = jnp.where(first, rz * 4 + rx, rx * 4 + rz)
            product = dot(w43[pl.ds(x * K, K), :], right).astype(BF)
            mm[:, slot] = product.reshape(16, 16, 512)

    def build(table, m):
        lanes = slice(m * EB, (m + 1) * EB)
        bc, bs = by_c[:, lanes], by_s[:, lanes]
        for wx in range(SIDE):
            ac, as_ = ax_c[wx : wx + 1, lanes], ax_s[wx : wx + 1, lanes]
            table[wx * 16 : wx * 16 + 16, 0:EB] = (ac * bc - as_ * bs).astype(BF)
            table[wx * 16 : wx * 16 + 16, EB : 2 * EB] = (as_ * bc + ac * bs).astype(BF)

    def multiply(table, m):
        sr = sig[0, m * EB : (m + 1) * EB, :]
        si = sig[1, m * EB : (m + 1) * EB, :]
        right = jnp.concatenate(
            [jnp.concatenate([sr, si], 1), jnp.concatenate([si, -sr], 1)], 0
        )
        c0[m] = dot(table[...], right)

    def along_x(my, part):
        for i in range(part * 8, part * 8 + 8):
            rows = slice(i * 8, i * 8 + 8)
            for half in range(2):
                re_at = slice(half * 128, half * 128 + 128)
                im_at = slice(COLS + half * 128, COLS + half * 128 + 128)
                x = [
                    (c0[my * 4 + mx, rows, re_at], c0[my * 4 + mx, rows, im_at])
                    for mx in range(4)
                ]
                for kx_, (re, im) in enumerate(dft4(x)):
                    c0[my * 4 + kx_, rows, re_at] = re
                    c0[my * 4 + kx_, rows, im_at] = im

    def along_y(kx_, part):
        for i in range(part * 4, part * 4 + 4):
            rows = slice(i * 16, i * 16 + 16)
            low = slice(K + i * 16, K + i * 16 + 16)
            for half in range(2):
                re_at = slice(half * 128, half * 128 + 128)
                im_at = slice(COLS + half * 128, COLS + half * 128 + 128)
                x = [
                    (c0[my * 4 + kx_, rows, re_at], c0[my * 4 + kx_, rows, im_at])
                    for my in range(4)
                ]
                for ky_, (re, im) in enumerate(dft4(x)):
                    re = (re * 0.25).astype(BF)
                    im = (im * 0.25).astype(BF)
                    cls = kx_ * 4 + ky_
                    d[cls, rows, re_at] = re
                    d[cls, rows, im_at] = im
                    d[cls, low, re_at] = -im
                    d[cls, low, im_at] = re

    def apply(cls):
        left = mm[cls].reshape(K, 2 * K)
        rows = slice(cls * 16, cls * 16 + 16)
        out = dot(left, d[cls]).astype(BF).reshape(4, 4, 16, 2 * COLS)
        p2hi[:, rows, :] = out[0, 0:2]
        p2lo[:, rows, :] = out[0, 2:4]
        q1u[:, rows, :] = out[1, 0:2]
        q1w[:, rows, :] = out[1, 2:4]
        qmw[:, rows, :] = out[2, 0:2]
        qmu[:, rows, :] = out[2, 2:4]
        own[:, rows, :] = out[3]

    tables = (t0, t1)
    build(t0, 0)
    for m in range(BOXES):
        if m % 4 == 0:
            s_copies[m // 4].wait()
        if m + 1 < BOXES:
            build(tables[(m + 1) % 2], m + 1)
        multiply(tables[m % 2], m)
        if m >= 4:
            along_x(m // 4 - 1, m % 4)
    for part in range(4):
        along_x(3, part)
    for part in range(4):
        along_y(0, part)
    for cls in range(16):
        if cls < 12:
            along_y(cls // 4 + 1, cls % 4)
        apply(cls)


def vm(n):
    return [pl.BlockSpec(memory_space=VMEM)] * n


def shaped(*dims, dtype=BF):
    return jax.ShapeDtypeStruct(dims, dtype)


def lead(positions, signal, weights):
    ne = positions.shape[1]
    hbm = pl.BlockSpec(memory_space=pltpu.HBM)
    return pl.pallas_call(
        lead_kernel,
        out_shape=[shaped(n, K, 2 * COLS) for n in (2, 2, 2, 2, 2, 2, 4)],
        in_specs=[hbm] * 3,
        out_specs=vm(7),
        scratch_shapes=[VMEM(positions.shape, jnp.int32), VMEM(signal.shape, BF), VMEM((4, 2, 2, K, K), BF)]
        + [VMEM((SIDE, ne), F32)] * 4
        + [VMEM((K, 2 * EB), BF)] * 2
        + [
            VMEM((BOXES, K, 2 * COLS), F32),
            VMEM((16, 2 * K, 2 * COLS), BF),
            VMEM((16, 16, 16, 2 * K), BF),
            VMEM((4 * K, 2 * K), BF),
            VMEM((4, 2 * K, 2 * K), BF),
            pltpu.SemaphoreType.DMA((5,)),
            pltpu.SemaphoreType.DMA((4,)),
        ],
        compiler_params=pltpu.CompilerParams(vmem_limit_bytes=48 << 20),
        cost_estimate=pl.CostEstimate(
            flops=8_000_000_000, transcendentals=0, bytes_accessed=12 << 20
        ),
        name="lead",
    )(positions, signal, weights)


def steer_kernel(pos, out, table):
    r = lax.broadcasted_iota(jnp.int32, (SIDE, 1), 0)
    n = pos.shape[-1]
    u, v = pos[0, 0:1, :], pos[1, 0:1, :]
    for kx in range(4):
        ac, as_ = sincos((r // 4 * 4 + kx - 8) * u)
        ac, as_ = ac * (1.0 / 16.0), as_ * (1.0 / 16.0)
        for ky in range(4):
            bc, bs = sincos((r % 4 * 4 + ky - 8) * v)
            rows = pl.ds((kx * 4 + ky) * 16, 16)
            table[rows, :] = ac * bc - as_ * bs
            table[pl.ds((kx * 4 + ky) * 16 + K, 16), :] = as_ * bc + ac * bs
    for i in range(n // 128):
        for j in range(2 * K // 128):
            block = table[pl.ds(j * 128, 128), pl.ds(i * 128, 128)]
            out[pl.ds(i * 128, 128), pl.ds(j * 128, 128)] = block.T.astype(BF)


def steer(directions):
    n = directions.shape[-1]
    return pl.pallas_call(
        steer_kernel,
        out_shape=shaped(n, 2 * K),
        in_specs=vm(1),
        out_specs=vm(1)[0],
        scratch_shapes=[VMEM((2 * K, n), F32)],
        cost_estimate=pl.CostEstimate(
            flops=1_500_000_000, transcendentals=0, bytes_accessed=1 << 20
        ),
        compiler_params=pltpu.CompilerParams(vmem_limit_bytes=16 << 20),
        name="steer",
    )(directions)


def added(*terms):
    total = terms[0].astype(F32)
    for t in terms[1:]:
        total = total + t.astype(F32)
    return total


def call(kernel, shapes, *args):
    return pl.pallas_call(
        kernel,
        out_shape=shapes,
        in_specs=vm(len(args)),
        out_specs=vm(len(shapes)),
        compiler_params=pltpu.CompilerParams(vmem_limit_bytes=24 << 20),
    )(*args)


def merge_kernel(mine, received, *outs):
    if len(outs) == 1:
        outs[0][...] = added(mine[...], received[...]).astype(BF)
    else:
        for i, o in enumerate(outs):
            o[...] = added(mine[i], received[i]).astype(BF)


def sum_far_kernel(own, g1, gm, lo, hi):
    s = added(own[0], g1[0], gm[...]).astype(BF)
    lo[...] = s[: K // 2]
    hi[...] = s[K // 2 :]


def sum_near_kernel(own, g1u, gmb, g1w, gmu, tlo, thi, u1, um, s0):
    h = K // 2
    one = added(own[1], g1u[1], gmb[...])
    u1[0:h] = (one[:h] + tlo[...].astype(F32)).astype(BF)
    u1[h:] = one[h:].astype(BF)
    other = added(own[2], g1w[0], gmu[0])
    um[0:h] = other[:h].astype(BF)
    um[h:] = (other[h:] + thi[...].astype(F32)).astype(BF)
    s0[...] = added(own[3], g1w[1], gmu[1])


def total_kernel(s0, v1, vm_, z):
    z[...] = added(s0[...], v1[...], vm_[...]).astype(BF)


def beam_kernel(offsets, table, *rest):
    parts = rest[: len(offsets)]
    out, buf, sem = rest[-3:]
    y = lax.axis_index("dir")
    n = table.shape[0] // 2
    copies = []
    for i, offset in enumerate(offsets):
        right = expand_right(parts[i][...])
        column = pl.multiple_of(jnp.bitwise_and(y + offset, 3) * COLS, COLS)
        for r in range(2):
            slot = len(copies) % 2
            if len(copies) >= 2:
                copies[-2].wait()
            b = dot(table[pl.ds(r * n, n), :], right).astype(BF)
            buf[slot, 0] = b[:, :COLS]
            buf[slot, 1] = b[:, COLS:]
            copies.append(
                pltpu.make_async_copy(
                    buf.at[slot],
                    out.at[:, 0, pl.ds(r * n, n), pl.ds(column, COLS)],
                    sem.at[slot],
                )
            )
            copies[-1].start()
    for c in copies[-2:]:
        c.wait()


def beams(offsets, table, parts, previous, shape):
    n = table.shape[0]
    hbm = pl.BlockSpec(memory_space=pltpu.HBM)
    extra = [] if previous is None else [previous]
    return pl.pallas_call(
        lambda *refs: beam_kernel(offsets, *refs),
        out_shape=jax.ShapeDtypeStruct(shape, BF),
        in_specs=vm(1 + len(parts)) + [hbm] * len(extra),
        out_specs=hbm,
        scratch_shapes=[
            VMEM((2, 2, n // 2, COLS), BF),
            pltpu.SemaphoreType.DMA((2,)),
        ],
        input_output_aliases={} if previous is None else {1 + len(parts): 0},
        cost_estimate=pl.CostEstimate(
            flops=2_000_000_000, transcendentals=0, bytes_accessed=1 << 20
        ),
        compiler_params=pltpu.CompilerParams(vmem_limit_bytes=24 << 20),
        name="beams",
    )(table, *parts, *extra)


def ring(step, first):
    pairs = []
    for z in range(4):
        for x in range(4):
            along_z = ((z + step) % 4) * 4 + x
            along_x = z * 4 + (x + step) % 4
            core0, core1 = (along_z, along_x) if first else (along_x, along_z)
            pairs.append((z * 4 + x, core0))
            pairs.append((16 + z * 4 + x, 16 + core1))
    return pairs


def local(signal, positions, weights, directions):
    along = ("freq", "z", "x")

    def major(a, step):
        return lax.ppermute(a, along, ring(step, True))

    def minor(a, step):
        return lax.ppermute(a, along, ring(step, False))

    def across(a, step):
        return lax.ppermute(a, "dir", [(i, (i + step) % 4) for i in range(4)])

    def compute():
        p2hi, p2lo, q1u, q1w, qmw, qmu, own = lead(positions, signal, weights)
        table = steer(directions)
        block = shaped(K, 2 * COLS)
        rhi, rlo = major(p2hi, -1), major(p2lo, 1)
        gmu, g1u = major(qmu, -1), major(q1u, 1)
        wma, wmb = call(merge_kernel, [block, block], qmw, rhi)
        (w1,) = call(merge_kernel, [shaped(2, K, 2 * COLS)], q1w, rlo)
        gma, g1w, gmb = major(wma, -1), major(w1, 1), major(wmb, -1)
        half = shaped(K // 2, 2 * COLS)
        lo, hi = call(sum_far_kernel, [half, half], own, g1u, gma)
        tlo, thi = minor(lo, 1), minor(hi, -1)
        u1, um, s0 = call(
            sum_near_kernel,
            [block, block, shaped(K, 2 * COLS, dtype=F32)],
            own, g1u, gmb, g1w, gmu, tlo, thi,
        )
        v1, v_m = minor(u1, 1), minor(um, -1)
        (zz,) = call(total_kernel, [block], s0, v1, v_m)
        y1, ym, y2 = across(zz, 1), across(zz, -1), across(zz, 2)
        shape = (2, 1, directions.shape[2], signal.shape[2] * 4)
        result = beams((0,), table, (zz,), None, shape)
        result = beams((3, 1), table, (y1, ym), result, shape)
        return beams((2,), table, (y2,), result, shape)

    return compute()


def solution(mesh):
    split = Mesh(mesh.devices.reshape(2, 4, 4, 4), ("freq", "dir", "z", "x"))
    ap = ("z", "x")
    in_specs = (P(None, ap, ("freq", "dir")), P(None, ap), P(), P(None, ap, "dir"))
    out_specs = P(None, ap, "dir", "freq")
    return jax.shard_map(
        local, mesh=split, in_specs=in_specs, out_specs=out_specs, check_vma=False
    )
```

```python
import math

import jax
import jax.numpy as jnp
from jax import lax
from jax.experimental import pallas as pl
from jax.experimental.pallas import tpu as pltpu
from jax.sharding import Mesh, PartitionSpec as P


K = 256
EB = 256
SIDE = 16
BOXES = 16
COLS = 256
F32 = jnp.float32
BF = jnp.bfloat16

LEAD_MIB = 34


def sincos(phase):
    p = jnp.bitwise_and(phase, 255)
    q = jnp.right_shift(p + 32, 6)
    t = (p - jnp.left_shift(q, 6)).astype(F32) * (2.0 * math.pi / 256.0)
    u = t * t
    s0 = t * (1.0 + u * (-1.0 / 6 + u * (1.0 / 120 + u * (-1.0 / 5040 + u * (1.0 / 362880)))))
    c0 = 1.0 + u * (-0.5 + u * (1.0 / 24 + u * (-1.0 / 720 + u * (1.0 / 40320))))
    odd = jnp.bitwise_and(q, 1) == 1
    c = jnp.where(odd, s0, c0)
    s = jnp.where(odd, c0, s0)
    c = jnp.where(jnp.bitwise_and(q + 1, 2) == 2, -c, c)
    s = jnp.where(jnp.bitwise_and(q, 2) == 2, -s, s)
    return c, s


def dot(a, b):
    return jnp.dot(a, b, preferred_element_type=F32)


OFFSETS = (2, 1, 3, 0)


def composites(mm, w43, e21, slots):
    core = lax.axis_index("freq")
    own_z, own_x = lax.axis_index("z"), lax.axis_index("x")
    for i, slot in enumerate(slots):
        major, minor = OFFSETS[slot // 4], OFFSETS[slot % 4]
        z = jnp.bitwise_and(own_z + jnp.where(core == 0, major, minor), 3)
        x = jnp.bitwise_and(own_x + jnp.where(core == 0, minor, major), 3)
        left = w43[pl.ds(pl.multiple_of(x * K, K), K), :]
        mm[:, i] = dot(left, e21[z]).astype(BF).reshape(16, 16, 2 * K)


def dft4(x):
    (a, b), (c, d), (e, f), (g, h) = x
    s0r, s0i, d0r, d0i = a + e, b + f, a - e, b - f
    s1r, s1i, d1r, d1i = c + g, d + h, c - g, d - h
    return (
        (s0r + s1r, s0i + s1i),
        (d0r + d1i, d0i - d1r),
        (s0r - s1r, s0i - s1i),
        (d0r - d1i, d0i + d1r),
    )


def expand_right(row_form):
    n = row_form.shape[-1] // 2
    r, i = row_form[:, :n], row_form[:, n:]
    return jnp.concatenate(
        [jnp.concatenate([r, i], 1), jnp.concatenate([-i, r], 1)], 0
    )


VMEM = pltpu.VMEM


def lead_kernel(pos_hbm, sig_hbm, w_hbm, *rest):
    p2hi, p2lo, d, w43, e21 = rest[:5]
    pos, sig, w, ax_c, ax_s, by_c, by_s, t0, t1, c0, mm, wsem, ssem = rest[5:]
    own_z, own_x = lax.axis_index("z"), lax.axis_index("x")
    child = (own_z // 2, own_z % 2, own_x // 2, own_x % 2)

    pos_copy = pltpu.make_async_copy(pos_hbm, pos, wsem.at[4])
    pos_copy.start()
    w_copies = [
        pltpu.make_async_copy(w_hbm.at[i, :, child[i]], w.at[i], wsem.at[i])
        for i in range(4)
    ]
    for i in (3, 2, 1, 0):
        w_copies[i].start()
    quarter = sig.shape[1] // 4
    s_copies = [
        pltpu.make_async_copy(
            sig_hbm.at[:, pl.ds(i * quarter, quarter), :],
            sig.at[:, pl.ds(i * quarter, quarter), :],
            ssem.at[i],
        )
        for i in range(4)
    ]
    for c in s_copies:
        c.start()

    pos_copy.wait()
    wave = lax.broadcasted_iota(jnp.int32, (SIDE, 1), 0) - SIDE // 2

    def factors(i, _):
        lanes = pl.ds(pl.multiple_of(i * 512, 512), 512)
        xc, xs = sincos(wave * pos[0:1, lanes])
        ax_c[:, lanes] = xc * (1.0 / 16.0)
        ax_s[:, lanes] = xs * (1.0 / 16.0)
        yc, ys = sincos(wave * pos[1:2, lanes])
        by_c[:, lanes] = yc
        by_s[:, lanes] = ys
        return 0

    lax.fori_loop(0, pos.shape[1] // 512, factors, 0)

    row = lax.broadcasted_iota(jnp.int32, (K, K), 0)
    col = lax.broadcasted_iota(jnp.int32, (K, K), 1)
    kx, ky = row // 64, row // 16 % 4
    hx, hy = row // 4 % 4, row % 4
    source = (hx * 4 + kx) * 16 + hy * 4 + ky
    pick = jnp.where(source == col, 1.0, 0.0).astype(BF)

    def row_form(level, r):
        return jnp.concatenate([w[level, r, 0], w[level, r, 1]], 1)

    w_copies[3].wait()
    upper = jnp.concatenate(
        [dot(pick, row_form(3, r)).astype(BF) for r in range(2)], 0
    )
    w_copies[2].wait()
    for r3 in range(2):
        w43[pl.ds(r3 * 512, 512), :] = dot(upper, expand_right(row_form(2, r3))).astype(BF)
    w_copies[1].wait()
    w_copies[0].wait()
    lower = jnp.concatenate([row_form(1, r) for r in range(2)], 0)
    for r1 in range(2):
        both = dot(lower, expand_right(row_form(0, r1))).astype(BF)
        for r2 in range(2):
            e21[r1 * 2 + r2] = expand_right(both[r2 * K : (r2 + 1) * K])

    composites(mm, w43, e21, range(4))

    def build(table, m):
        lanes = slice(m * EB, (m + 1) * EB)
        bc, bs = by_c[:, lanes], by_s[:, lanes]
        for wx in range(SIDE):
            ac, as_ = ax_c[wx : wx + 1, lanes], ax_s[wx : wx + 1, lanes]
            table[wx * 16 : wx * 16 + 16, 0:EB] = (ac * bc - as_ * bs).astype(BF)
            table[wx * 16 : wx * 16 + 16, EB : 2 * EB] = (as_ * bc + ac * bs).astype(BF)

    def multiply(table, m):
        sr = sig[0, m * EB : (m + 1) * EB, :]
        si = sig[1, m * EB : (m + 1) * EB, :]
        right = jnp.concatenate(
            [jnp.concatenate([sr, si], 1), jnp.concatenate([si, -sr], 1)], 0
        )
        c0[m] = dot(table[...], right)

    def along_x(my, part):
        for i in range(part * 8, part * 8 + 8):
            rows = slice(i * 8, i * 8 + 8)
            for half in range(2):
                re_at = slice(half * 128, half * 128 + 128)
                im_at = slice(COLS + half * 128, COLS + half * 128 + 128)
                x = [
                    (c0[my * 4 + mx, rows, re_at], c0[my * 4 + mx, rows, im_at])
                    for mx in range(4)
                ]
                for kx_, (re, im) in enumerate(dft4(x)):
                    c0[my * 4 + kx_, rows, re_at] = re
                    c0[my * 4 + kx_, rows, im_at] = im

    def along_y(kx_, part):
        for i in range(part * 4, part * 4 + 4):
            rows = slice(i * 16, i * 16 + 16)
            low = slice(K + i * 16, K + i * 16 + 16)
            for half in range(2):
                re_at = slice(half * 128, half * 128 + 128)
                im_at = slice(COLS + half * 128, COLS + half * 128 + 128)
                x = [
                    (c0[my * 4 + kx_, rows, re_at], c0[my * 4 + kx_, rows, im_at])
                    for my in range(4)
                ]
                for ky_, (re, im) in enumerate(dft4(x)):
                    re = (re * 0.25).astype(BF)
                    im = (im * 0.25).astype(BF)
                    cls = kx_ * 4 + ky_
                    d[cls, rows, re_at] = re
                    d[cls, rows, im_at] = im
                    d[cls, low, re_at] = -im
                    d[cls, low, im_at] = re

    def apply(cls):
        rows = slice(cls * 16, cls * 16 + 16)
        out = dot(mm[cls].reshape(K // 4, 2 * K), d[cls]).astype(BF).reshape(4, 16, 2 * COLS)
        p2hi[:, rows, :] = out[0:2]
        p2lo[:, rows, :] = out[2:4]

    tables = (t0, t1)
    build(t0, 0)
    for m in range(BOXES):
        if m % 4 == 0:
            s_copies[m // 4].wait()
        if m + 1 < BOXES:
            build(tables[(m + 1) % 2], m + 1)
        multiply(tables[m % 2], m)
        if m >= 4:
            along_x(m // 4 - 1, m % 4)
    for part in range(4):
        along_x(3, part)
    for part in range(4):
        along_y(0, part)
    for cls in range(16):
        if cls < 12:
            along_y(cls // 4 + 1, cls % 4)
        apply(cls)


def vm(n):
    return [pl.BlockSpec(memory_space=VMEM)] * n


def shaped(*dims, dtype=BF):
    return jax.ShapeDtypeStruct(dims, dtype)


def rest_kernel(d, w43, e21, *refs):
    q1f, q1n, qmf, qmn, own, mm = refs
    composites(mm, w43, e21, range(4, 16))
    for cls in range(16):
        rows = slice(cls * 16, cls * 16 + 16)
        out = dot(mm[cls].reshape(3 * K // 4, 2 * K), d[cls]).astype(BF)
        out = out.reshape(3, 4, 16, 2 * COLS)
        q1f[rows, :] = out[0, 0]
        q1n[:, rows, :] = out[0, 1:4]
        qmf[rows, :] = out[1, 0]
        qmn[:, rows, :] = out[1, 1:4]
        own[:, rows, :] = out[2]


def lead(positions, signal, weights):
    ne = positions.shape[1]
    hbm = pl.BlockSpec(memory_space=pltpu.HBM)
    far = pl.pallas_call(
        lead_kernel,
        out_shape=[shaped(2, K, 2 * COLS)] * 2
        + [shaped(16, 2 * K, 2 * COLS), shaped(4 * K, 2 * K), shaped(4, 2 * K, 2 * K)],
        in_specs=[hbm] * 3,
        out_specs=vm(5),
        scratch_shapes=[
            VMEM(positions.shape, jnp.int32),
            VMEM(signal.shape, BF),
            VMEM((4, 2, 2, K, K), BF),
        ]
        + [VMEM((SIDE, ne), F32)] * 4
        + [VMEM((K, 2 * EB), BF)] * 2
        + [
            VMEM((BOXES, K, 2 * COLS), F32),
            VMEM((16, 4, 16, 2 * K), BF),
            pltpu.SemaphoreType.DMA((5,)),
            pltpu.SemaphoreType.DMA((4,)),
        ],
        compiler_params=pltpu.CompilerParams(vmem_limit_bytes=LEAD_MIB << 20),
        cost_estimate=pl.CostEstimate(
            flops=8_000_000_000, transcendentals=0, bytes_accessed=12 << 20
        ),
        name="lead",
    )(*(pltpu.with_memory_space_constraint(a, pltpu.HBM) for a in (positions, signal, weights)))
    p2hi, p2lo, d, w43, e21 = far
    near = pl.pallas_call(
        rest_kernel,
        out_shape=[
            shaped(*n, K, 2 * COLS) for n in ((), (3,), (), (3,), (4,))
        ],
        in_specs=vm(3),
        out_specs=vm(5),
        scratch_shapes=[VMEM((16, 12, 16, 2 * K), BF)],
        compiler_params=pltpu.CompilerParams(vmem_limit_bytes=30 << 20),
        cost_estimate=pl.CostEstimate(
            flops=3_000_000_000, transcendentals=0, bytes_accessed=12 << 20
        ),
        name="rest",
    )(d, w43, e21)
    return p2hi, p2lo, *near


def steer_kernel(pos, out, table):
    r = lax.broadcasted_iota(jnp.int32, (SIDE, 1), 0)
    n = pos.shape[-1]
    u, v = pos[0, 0:1, :], pos[1, 0:1, :]
    for kx in range(4):
        ac, as_ = sincos((r // 4 * 4 + kx - 8) * u)
        ac, as_ = ac * (1.0 / 16.0), as_ * (1.0 / 16.0)
        for ky in range(4):
            bc, bs = sincos((r % 4 * 4 + ky - 8) * v)
            rows = pl.ds((kx * 4 + ky) * 16, 16)
            table[rows, :] = ac * bc - as_ * bs
            table[pl.ds((kx * 4 + ky) * 16 + K, 16), :] = as_ * bc + ac * bs
    for i in range(n // 128):
        for j in range(2 * K // 128):
            block = table[pl.ds(j * 128, 128), pl.ds(i * 128, 128)]
            out[pl.ds(i * 128, 128), pl.ds(j * 128, 128)] = block.T.astype(BF)


def steer(directions):
    n = directions.shape[-1]
    return pl.pallas_call(
        steer_kernel,
        out_shape=shaped(n, 2 * K),
        in_specs=vm(1),
        out_specs=vm(1)[0],
        scratch_shapes=[VMEM((2 * K, n), F32)],
        cost_estimate=pl.CostEstimate(
            flops=1_500_000_000, transcendentals=0, bytes_accessed=1 << 20
        ),
        compiler_params=pltpu.CompilerParams(vmem_limit_bytes=16 << 20),
        name="steer",
    )(directions)


def added(*terms):
    total = terms[0].astype(F32)
    for t in terms[1:]:
        total = total + t.astype(F32)
    return total


def call(kernel, shapes, *args):
    return pl.pallas_call(
        kernel,
        out_shape=shapes,
        in_specs=vm(len(args)),
        out_specs=vm(len(shapes)),
        compiler_params=pltpu.CompilerParams(vmem_limit_bytes=24 << 20),
    )(*args)


def merge_down_kernel(far, near, received, out_far, out_near):
    out_far[...] = added(far[...], received[0]).astype(BF)
    out_near[0] = added(near[0], received[1]).astype(BF)
    out_near[1:3] = near[1:3]


def merge_up_kernel(near, received, out_near):
    out_near[0] = near[0]
    out_near[1:3] = added(near[1:3], received[...]).astype(BF)


def sum_far_kernel(own, up, down, out):
    out[...] = added(own[0], up[...], down[...]).astype(BF)


def sum_near_kernel(own, up, down, u1, um, s0):
    u1[...] = added(own[1], up[0], down[0]).astype(BF)
    um[...] = added(own[2], up[1], down[1]).astype(BF)
    s0[...] = added(own[3], up[2], down[2])


def total_kernel(s0, t2, v1, v_m, z):
    z[...] = added(s0[...], t2[...], v1[...], v_m[...]).astype(BF)


def beam_kernel(offsets, table, *rest):
    parts = rest[: len(offsets)]
    out, buf, sem = rest[-3:]
    y = lax.axis_index("dir")
    n = table.shape[0] // 2
    copies = []
    for i, offset in enumerate(offsets):
        right = expand_right(parts[i][...])
        column = pl.multiple_of(jnp.bitwise_and(y + offset, 3) * COLS, COLS)
        for r in range(2):
            slot = len(copies) % 2
            if len(copies) >= 2:
                copies[-2].wait()
            b = dot(table[pl.ds(r * n, n), :], right).astype(BF)
            buf[slot, 0] = b[:, :COLS]
            buf[slot, 1] = b[:, COLS:]
            copies.append(
                pltpu.make_async_copy(
                    buf.at[slot],
                    out.at[:, 0, pl.ds(r * n, n), pl.ds(column, COLS)],
                    sem.at[slot],
                )
            )
            copies[-1].start()
    for c in copies[-2:]:
        c.wait()


def beams(offsets, table, parts, previous, shape):
    n = table.shape[0]
    hbm = pl.BlockSpec(memory_space=pltpu.HBM)
    extra = [] if previous is None else [previous]
    return pl.pallas_call(
        lambda *refs: beam_kernel(offsets, *refs),
        out_shape=jax.ShapeDtypeStruct(shape, BF),
        in_specs=vm(1 + len(parts)) + [hbm] * len(extra),
        out_specs=hbm,
        scratch_shapes=[
            VMEM((2, 2, n // 2, COLS), BF),
            pltpu.SemaphoreType.DMA((2,)),
        ],
        input_output_aliases={} if previous is None else {1 + len(parts): 0},
        cost_estimate=pl.CostEstimate(
            flops=2_000_000_000, transcendentals=0, bytes_accessed=1 << 20
        ),
        compiler_params=pltpu.CompilerParams(vmem_limit_bytes=24 << 20),
        name="beams",
    )(table, *parts, *extra)


def ring(step, first):
    pairs = []
    for z in range(4):
        for x in range(4):
            along_z = ((z + step) % 4) * 4 + x
            along_x = z * 4 + (x + step) % 4
            core0, core1 = (along_z, along_x) if first else (along_x, along_z)
            pairs.append((z * 4 + x, core0))
            pairs.append((16 + z * 4 + x, 16 + core1))
    return pairs


def local(signal, positions, weights, directions):
    along = ("freq", "z", "x")

    def major(a, step):
        return lax.ppermute(a, along, ring(step, True))

    def minor(a, step):
        return lax.ppermute(a, along, ring(step, False))

    def across(a, step):
        return lax.ppermute(a, "dir", [(i, (i + step) % 4) for i in range(4)])

    def compute():
        p2hi, p2lo, q1f, q1n, qmf, qmn, own = lead(positions, signal, weights)
        table = steer(directions)
        block, three = shaped(K, 2 * COLS), shaped(3, K, 2 * COLS)
        rhi, rlo = major(p2hi, -1), major(p2lo, 1)
        up_far = major(q1f, 1)
        wmf, wmn = call(merge_down_kernel, [block, three], qmf, qmn, rhi)
        down_far = major(wmf, -1)
        down_near = major(wmn, -1)
        (w1n,) = call(merge_up_kernel, [three], q1n, rlo)
        up_near = major(w1n, 1)
        (far,) = call(sum_far_kernel, [block], own, up_far, down_far)
        t2 = minor(far, 2)
        u1, um, s0 = call(
            sum_near_kernel,
            [block, block, shaped(K, 2 * COLS, dtype=F32)],
            own, up_near, down_near,
        )
        v1, v_m = minor(u1, 1), minor(um, -1)
        (zz,) = call(total_kernel, [block], s0, t2, v1, v_m)
        y1, ym, y2 = across(zz, 1), across(zz, -1), across(zz, 2)
        shape = (2, 1, directions.shape[2], signal.shape[2] * 4)
        result = beams((0,), table, (zz,), None, shape)
        result = beams((3, 1), table, (y1, ym), result, shape)
        return beams((2,), table, (y2,), result, shape)

    return compute()


def solution(mesh):
    split = Mesh(mesh.devices.reshape(2, 4, 4, 4), ("freq", "dir", "z", "x"))
    ap = ("z", "x")
    in_specs = (P(None, ap, ("freq", "dir")), P(None, ap), P(), P(None, ap, "dir"))
    out_specs = P(None, ap, "dir", "freq")
    return jax.shard_map(
        local, mesh=split, in_specs=in_specs, out_specs=out_specs, check_vma=False
    )
```

```python
import math

import jax
import jax.numpy as jnp
from jax import lax
from jax.experimental import pallas as pl
from jax.experimental.pallas import tpu as pltpu
from jax.sharding import Mesh, PartitionSpec as P


K = 256
EB = 256
SIDE = 16
BOXES = 16
COLS = 256
F32 = jnp.float32
BF = jnp.bfloat16

LEAD_MIB = 34


def sincos(phase):
    p = jnp.bitwise_and(phase, 255)
    q = jnp.right_shift(p + 32, 6)
    t = (p - jnp.left_shift(q, 6)).astype(F32) * (2.0 * math.pi / 256.0)
    u = t * t
    s0 = t * (1.0 + u * (-1.0 / 6 + u * (1.0 / 120 + u * (-1.0 / 5040 + u * (1.0 / 362880)))))
    c0 = 1.0 + u * (-0.5 + u * (1.0 / 24 + u * (-1.0 / 720 + u * (1.0 / 40320))))
    odd = jnp.bitwise_and(q, 1) == 1
    c = jnp.where(odd, s0, c0)
    s = jnp.where(odd, c0, s0)
    c = jnp.where(jnp.bitwise_and(q + 1, 2) == 2, -c, c)
    s = jnp.where(jnp.bitwise_and(q, 2) == 2, -s, s)
    return c, s


def dot(a, b):
    return jnp.dot(a, b, preferred_element_type=F32)


OFFSETS = (2, 1, 3, 0)


def composites(mm, w43, e21, slots):
    core = lax.axis_index("freq")
    own_z, own_x = lax.axis_index("z"), lax.axis_index("x")
    for i, slot in enumerate(slots):
        major, minor = OFFSETS[slot // 4], OFFSETS[slot % 4]
        z = jnp.bitwise_and(own_z + jnp.where(core == 0, major, minor), 3)
        x = jnp.bitwise_and(own_x + jnp.where(core == 0, minor, major), 3)
        left = w43[pl.ds(pl.multiple_of(x * K, K), K), :]
        mm[:, i] = dot(left, e21[z]).astype(BF).reshape(16, 16, 2 * K)


def dft4(x):
    (a, b), (c, d), (e, f), (g, h) = x
    s0r, s0i, d0r, d0i = a + e, b + f, a - e, b - f
    s1r, s1i, d1r, d1i = c + g, d + h, c - g, d - h
    return (
        (s0r + s1r, s0i + s1i),
        (d0r + d1i, d0i - d1r),
        (s0r - s1r, s0i - s1i),
        (d0r - d1i, d0i + d1r),
    )


def expand_right(row_form):
    n = row_form.shape[-1] // 2
    r, i = row_form[:, :n], row_form[:, n:]
    return jnp.concatenate(
        [jnp.concatenate([r, i], 1), jnp.concatenate([-i, r], 1)], 0
    )


VMEM = pltpu.VMEM


def lead_kernel(pos_hbm, sig_hbm, w_hbm, *rest):
    p2hi, p2lo, d, w43, e21 = rest[:5]
    pos, sig, w, ax_c, ax_s, by_c, by_s, t0, t1, c0, mm, wsem, ssem = rest[5:]
    own_z, own_x = lax.axis_index("z"), lax.axis_index("x")
    child = (own_z // 2, own_z % 2, own_x // 2, own_x % 2)

    pos_copy = pltpu.make_async_copy(pos_hbm, pos, wsem.at[4])
    pos_copy.start()
    w_copies = [
        pltpu.make_async_copy(w_hbm.at[i, :, child[i]], w.at[i], wsem.at[i])
        for i in range(4)
    ]
    for i in (3, 2, 1, 0):
        w_copies[i].start()
    quarter = sig.shape[1] // 4
    s_copies = [
        pltpu.make_async_copy(
            sig_hbm.at[:, pl.ds(i * quarter, quarter), :],
            sig.at[:, pl.ds(i * quarter, quarter), :],
            ssem.at[i],
        )
        for i in range(4)
    ]
    for c in s_copies:
        c.start()

    pos_copy.wait()
    wave = lax.broadcasted_iota(jnp.int32, (SIDE, 1), 0) - SIDE // 2

    def factors(i, _):
        lanes = pl.ds(pl.multiple_of(i * 512, 512), 512)
        xc, xs = sincos(wave * pos[0:1, lanes])
        ax_c[:, lanes] = xc * (1.0 / 16.0)
        ax_s[:, lanes] = xs * (1.0 / 16.0)
        yc, ys = sincos(wave * pos[1:2, lanes])
        by_c[:, lanes] = yc
        by_s[:, lanes] = ys
        return 0

    lax.fori_loop(0, pos.shape[1] // 512, factors, 0)

    row = lax.broadcasted_iota(jnp.int32, (K, K), 0)
    col = lax.broadcasted_iota(jnp.int32, (K, K), 1)
    kx, ky = row // 64, row // 16 % 4
    hx, hy = row // 4 % 4, row % 4
    source = (hx * 4 + kx) * 16 + hy * 4 + ky
    pick = jnp.where(source == col, 1.0, 0.0).astype(BF)

    def row_form(level, r):
        return jnp.concatenate([w[level, r, 0], w[level, r, 1]], 1)

    w_copies[3].wait()
    upper = jnp.concatenate(
        [dot(pick, row_form(3, r)).astype(BF) for r in range(2)], 0
    )
    w_copies[2].wait()
    for r3 in range(2):
        w43[pl.ds(r3 * 512, 512), :] = dot(upper, expand_right(row_form(2, r3))).astype(BF)
    w_copies[1].wait()
    w_copies[0].wait()
    lower = jnp.concatenate([row_form(1, r) for r in range(2)], 0)
    for r1 in range(2):
        both = dot(lower, expand_right(row_form(0, r1))).astype(BF)
        for r2 in range(2):
            e21[r1 * 2 + r2] = expand_right(both[r2 * K : (r2 + 1) * K])

    composites(mm, w43, e21, range(4))

    def build(table, m):
        lanes = slice(m * EB, (m + 1) * EB)
        bc, bs = by_c[:, lanes], by_s[:, lanes]
        for wx in range(SIDE):
            ac, as_ = ax_c[wx : wx + 1, lanes], ax_s[wx : wx + 1, lanes]
            table[wx * 16 : wx * 16 + 16, 0:EB] = (ac * bc - as_ * bs).astype(BF)
            table[wx * 16 : wx * 16 + 16, EB : 2 * EB] = (as_ * bc + ac * bs).astype(BF)

    def multiply(table, m):
        sr = sig[0, m * EB : (m + 1) * EB, :]
        si = sig[1, m * EB : (m + 1) * EB, :]
        right = jnp.concatenate(
            [jnp.concatenate([sr, si], 1), jnp.concatenate([si, -sr], 1)], 0
        )
        c0[m] = dot(table[...], right)

    def along_x(my, part):
        for i in range(part * 8, part * 8 + 8):
            rows = slice(i * 8, i * 8 + 8)
            for half in range(2):
                re_at = slice(half * 128, half * 128 + 128)
                im_at = slice(COLS + half * 128, COLS + half * 128 + 128)
                x = [
                    (c0[my * 4 + mx, rows, re_at], c0[my * 4 + mx, rows, im_at])
                    for mx in range(4)
                ]
                for kx_, (re, im) in enumerate(dft4(x)):
                    c0[my * 4 + kx_, rows, re_at] = re
                    c0[my * 4 + kx_, rows, im_at] = im

    def along_y(kx_, part):
        for i in range(part * 4, part * 4 + 4):
            rows = slice(i * 16, i * 16 + 16)
            low = slice(K + i * 16, K + i * 16 + 16)
            for half in range(2):
                re_at = slice(half * 128, half * 128 + 128)
                im_at = slice(COLS + half * 128, COLS + half * 128 + 128)
                x = [
                    (c0[my * 4 + kx_, rows, re_at], c0[my * 4 + kx_, rows, im_at])
                    for my in range(4)
                ]
                for ky_, (re, im) in enumerate(dft4(x)):
                    re = (re * 0.25).astype(BF)
                    im = (im * 0.25).astype(BF)
                    cls = kx_ * 4 + ky_
                    d[cls, rows, re_at] = re
                    d[cls, rows, im_at] = im
                    d[cls, low, re_at] = -im
                    d[cls, low, im_at] = re

    def apply(cls):
        rows = slice(cls * 16, cls * 16 + 16)
        out = dot(mm[cls].reshape(K // 4, 2 * K), d[cls]).astype(BF).reshape(4, 16, 2 * COLS)
        p2hi[:, rows, :] = out[0:2]
        p2lo[:, rows, :] = out[2:4]

    tables = (t0, t1)
    build(t0, 0)
    for m in range(BOXES):
        if m % 4 == 0:
            s_copies[m // 4].wait()
        if m + 1 < BOXES:
            build(tables[(m + 1) % 2], m + 1)
        multiply(tables[m % 2], m)
        if m >= 4:
            along_x(m // 4 - 1, m % 4)
    for part in range(4):
        along_x(3, part)
    for part in range(4):
        along_y(0, part)
    for cls in range(16):
        if cls < 12:
            along_y(cls // 4 + 1, cls % 4)
        apply(cls)


def vm(n):
    return [pl.BlockSpec(memory_space=VMEM)] * n


def shaped(*dims, dtype=BF):
    return jax.ShapeDtypeStruct(dims, dtype)


def rest_kernel(d, w43, e21, *refs):
    q1f, q1n, qmf, qmn, own, mm = refs
    composites(mm, w43, e21, range(4, 16))
    for cls in range(16):
        rows = slice(cls * 16, cls * 16 + 16)
        out = dot(mm[cls].reshape(3 * K // 4, 2 * K), d[cls]).astype(BF)
        out = out.reshape(3, 4, 16, 2 * COLS)
        q1f[rows, :] = out[0, 0]
        q1n[:, rows, :] = out[0, 1:4]
        qmf[rows, :] = out[1, 0]
        qmn[:, rows, :] = out[1, 1:4]
        own[:, rows, :] = out[2]


def lead(positions, signal, weights):
    ne = positions.shape[1]
    hbm = pl.BlockSpec(memory_space=pltpu.HBM)
    far = pl.pallas_call(
        lead_kernel,
        out_shape=[shaped(2, K, 2 * COLS)] * 2
        + [shaped(16, 2 * K, 2 * COLS), shaped(4 * K, 2 * K), shaped(4, 2 * K, 2 * K)],
        in_specs=[hbm] * 3,
        out_specs=vm(5),
        scratch_shapes=[
            VMEM(positions.shape, jnp.int32),
            VMEM(signal.shape, BF),
            VMEM((4, 2, 2, K, K), BF),
        ]
        + [VMEM((SIDE, ne), F32)] * 4
        + [VMEM((K, 2 * EB), BF)] * 2
        + [
            VMEM((BOXES, K, 2 * COLS), F32),
            VMEM((16, 4, 16, 2 * K), BF),
            pltpu.SemaphoreType.DMA((5,)),
            pltpu.SemaphoreType.DMA((4,)),
        ],
        compiler_params=pltpu.CompilerParams(vmem_limit_bytes=LEAD_MIB << 20),
        cost_estimate=pl.CostEstimate(
            flops=8_000_000_000, transcendentals=0, bytes_accessed=12 << 20
        ),
        name="lead",
    )(*(pltpu.with_memory_space_constraint(a, pltpu.HBM) for a in (positions, signal, weights)))
    p2hi, p2lo, d, w43, e21 = far
    near = pl.pallas_call(
        rest_kernel,
        out_shape=[
            shaped(*n, K, 2 * COLS) for n in ((), (3,), (), (3,), (4,))
        ],
        in_specs=vm(3),
        out_specs=vm(5),
        scratch_shapes=[VMEM((16, 12, 16, 2 * K), BF)],
        compiler_params=pltpu.CompilerParams(vmem_limit_bytes=30 << 20),
        cost_estimate=pl.CostEstimate(
            flops=3_000_000_000, transcendentals=0, bytes_accessed=12 << 20
        ),
        name="rest",
    )(d, w43, e21)
    return p2hi, p2lo, *near


def steer_kernel(pos, out, table):
    r = lax.broadcasted_iota(jnp.int32, (SIDE, 1), 0)
    n = pos.shape[-1]
    u, v = pos[0, 0:1, :], pos[1, 0:1, :]
    for kx in range(4):
        ac, as_ = sincos((r // 4 * 4 + kx - 8) * u)
        ac, as_ = ac * (1.0 / 16.0), as_ * (1.0 / 16.0)
        for ky in range(4):
            bc, bs = sincos((r % 4 * 4 + ky - 8) * v)
            rows = pl.ds((kx * 4 + ky) * 16, 16)
            table[rows, :] = ac * bc - as_ * bs
            table[pl.ds((kx * 4 + ky) * 16 + K, 16), :] = as_ * bc + ac * bs
    for i in range(n // 128):
        for j in range(2 * K // 128):
            block = table[pl.ds(j * 128, 128), pl.ds(i * 128, 128)]
            out[pl.ds(i * 128, 128), pl.ds(j * 128, 128)] = block.T.astype(BF)


def steer(directions):
    n = directions.shape[-1]
    return pl.pallas_call(
        steer_kernel,
        out_shape=shaped(n, 2 * K),
        in_specs=vm(1),
        out_specs=vm(1)[0],
        scratch_shapes=[VMEM((2 * K, n), F32)],
        cost_estimate=pl.CostEstimate(
            flops=1_500_000_000, transcendentals=0, bytes_accessed=1 << 20
        ),
        compiler_params=pltpu.CompilerParams(vmem_limit_bytes=16 << 20),
        name="steer",
    )(directions)


def added(*terms):
    total = terms[0].astype(F32)
    for t in terms[1:]:
        total = total + t.astype(F32)
    return total


def call(kernel, shapes, *args):
    return pl.pallas_call(
        kernel,
        out_shape=shapes,
        in_specs=vm(len(args)),
        out_specs=vm(len(shapes)),
        compiler_params=pltpu.CompilerParams(vmem_limit_bytes=24 << 20),
    )(*args)


def merge_down_kernel(far, near, received, out_far, out_near):
    out_far[...] = added(far[...], received[0]).astype(BF)
    out_near[0] = added(near[0], received[1]).astype(BF)
    out_near[1:3] = near[1:3]


def merge_up_kernel(near, received, out_near):
    out_near[0] = near[0]
    out_near[1:3] = added(near[1:3], received[...]).astype(BF)


def sum_far_kernel(own, up, down, lo, hi):
    s = added(own[0], up[...], down[...]).astype(BF)
    lo[...] = s[: K // 2]
    hi[...] = s[K // 2 :]


def sum_near_kernel(own, up, down, tlo, thi, u1, um, s0):
    h = K // 2
    one = added(own[1], up[0], down[0])
    u1[0:h] = (one[:h] + tlo[...].astype(F32)).astype(BF)
    u1[h:] = one[h:].astype(BF)
    other = added(own[2], up[1], down[1])
    um[0:h] = other[:h].astype(BF)
    um[h:] = (other[h:] + thi[...].astype(F32)).astype(BF)
    s0[...] = added(own[3], up[2], down[2])


def total_kernel(s0, v1, v_m, z):
    z[...] = added(s0[...], v1[...], v_m[...]).astype(BF)


def beam_kernel(offsets, table, *rest):
    parts = rest[: len(offsets)]
    out, buf, sem = rest[-3:]
    y = lax.axis_index("dir")
    n = table.shape[0] // 2
    copies = []
    for i, offset in enumerate(offsets):
        right = expand_right(parts[i][...])
        column = pl.multiple_of(jnp.bitwise_and(y + offset, 3) * COLS, COLS)
        for r in range(2):
            slot = len(copies) % 2
            if len(copies) >= 2:
                copies[-2].wait()
            b = dot(table[pl.ds(r * n, n), :], right).astype(BF)
            buf[slot, 0] = b[:, :COLS]
            buf[slot, 1] = b[:, COLS:]
            copies.append(
                pltpu.make_async_copy(
                    buf.at[slot],
                    out.at[:, 0, pl.ds(r * n, n), pl.ds(column, COLS)],
                    sem.at[slot],
                )
            )
            copies[-1].start()
    for c in copies[-2:]:
        c.wait()


def beams(offsets, table, parts, previous, shape):
    n = table.shape[0]
    hbm = pl.BlockSpec(memory_space=pltpu.HBM)
    extra = [] if previous is None else [previous]
    return pl.pallas_call(
        lambda *refs: beam_kernel(offsets, *refs),
        out_shape=jax.ShapeDtypeStruct(shape, BF),
        in_specs=vm(1 + len(parts)) + [hbm] * len(extra),
        out_specs=hbm,
        scratch_shapes=[
            VMEM((2, 2, n // 2, COLS), BF),
            pltpu.SemaphoreType.DMA((2,)),
        ],
        input_output_aliases={} if previous is None else {1 + len(parts): 0},
        cost_estimate=pl.CostEstimate(
            flops=2_000_000_000, transcendentals=0, bytes_accessed=1 << 20
        ),
        compiler_params=pltpu.CompilerParams(vmem_limit_bytes=24 << 20),
        name="beams",
    )(table, *parts, *extra)


def ring(step, first):
    pairs = []
    for z in range(4):
        for x in range(4):
            along_z = ((z + step) % 4) * 4 + x
            along_x = z * 4 + (x + step) % 4
            core0, core1 = (along_z, along_x) if first else (along_x, along_z)
            pairs.append((z * 4 + x, core0))
            pairs.append((16 + z * 4 + x, 16 + core1))
    return pairs


def local(signal, positions, weights, directions):
    along = ("freq", "z", "x")

    def major(a, step):
        return lax.ppermute(a, along, ring(step, True))

    def minor(a, step):
        return lax.ppermute(a, along, ring(step, False))

    def across(a, step):
        return lax.ppermute(a, "dir", [(i, (i + step) % 4) for i in range(4)])

    def compute():
        p2hi, p2lo, q1f, q1n, qmf, qmn, own = lead(positions, signal, weights)
        table = steer(directions)
        block, three = shaped(K, 2 * COLS), shaped(3, K, 2 * COLS)
        rhi, rlo = major(p2hi, -1), major(p2lo, 1)
        up_far = major(q1f, 1)
        wmf, wmn = call(merge_down_kernel, [block, three], qmf, qmn, rhi)
        down_far = major(wmf, -1)
        down_near = major(wmn, -1)
        (w1n,) = call(merge_up_kernel, [three], q1n, rlo)
        up_near = major(w1n, 1)
        half = shaped(K // 2, 2 * COLS)
        lo, hi = call(sum_far_kernel, [half, half], own, up_far, down_far)
        tlo, thi = minor(lo, 1), minor(hi, -1)
        u1, um, s0 = call(
            sum_near_kernel,
            [block, block, shaped(K, 2 * COLS, dtype=F32)],
            own, up_near, down_near, tlo, thi,
        )
        v1, v_m = minor(u1, 1), minor(um, -1)
        (zz,) = call(total_kernel, [block], s0, v1, v_m)
        y1, ym, y2 = across(zz, 1), across(zz, -1), across(zz, 2)
        shape = (2, 1, directions.shape[2], signal.shape[2] * 4)
        result = beams((0,), table, (zz,), None, shape)
        result = beams((3, 1), table, (y1, ym), result, shape)
        return beams((2,), table, (y2,), result, shape)

    return compute()


def solution(mesh):
    split = Mesh(mesh.devices.reshape(2, 4, 4, 4), ("freq", "dir", "z", "x"))
    ap = ("z", "x")
    in_specs = (P(None, ap, ("freq", "dir")), P(None, ap), P(), P(None, ap, "dir"))
    out_specs = P(None, ap, "dir", "freq")
    return jax.shard_map(
        local, mesh=split, in_specs=in_specs, out_specs=out_specs, check_vma=False
    )
```

```python
import math

import jax
import jax.numpy as jnp
from jax import lax
from jax.experimental import pallas as pl
from jax.experimental.pallas import tpu as pltpu
from jax.sharding import Mesh, PartitionSpec as P


K = 256
EB = 256
SIDE = 16
BOXES = 16
COLS = 256
F32 = jnp.float32
BF = jnp.bfloat16

LEAD_MIB = 34


def sincos(phase):
    p = jnp.bitwise_and(phase, 255)
    q = jnp.right_shift(p + 32, 6)
    t = (p - jnp.left_shift(q, 6)).astype(F32) * (2.0 * math.pi / 256.0)
    u = t * t
    s0 = t * (1.0 + u * (-1.0 / 6 + u * (1.0 / 120 + u * (-1.0 / 5040 + u * (1.0 / 362880)))))
    c0 = 1.0 + u * (-0.5 + u * (1.0 / 24 + u * (-1.0 / 720 + u * (1.0 / 40320))))
    odd = jnp.bitwise_and(q, 1) == 1
    c = jnp.where(odd, s0, c0)
    s = jnp.where(odd, c0, s0)
    c = jnp.where(jnp.bitwise_and(q + 1, 2) == 2, -c, c)
    s = jnp.where(jnp.bitwise_and(q, 2) == 2, -s, s)
    return c, s


def dot(a, b):
    return jnp.dot(a, b, preferred_element_type=F32)


OFFSETS = (2, 1, 3, 0)


def composites(mm, w43, e21, slots):
    core = lax.axis_index("freq")
    own_z, own_x = lax.axis_index("z"), lax.axis_index("x")
    for i, slot in enumerate(slots):
        major, minor = OFFSETS[slot // 4], OFFSETS[slot % 4]
        z = jnp.bitwise_and(own_z + jnp.where(core == 0, major, minor), 3)
        x = jnp.bitwise_and(own_x + jnp.where(core == 0, minor, major), 3)
        left = w43[pl.ds(pl.multiple_of(x * K, K), K), :]
        mm[:, i] = dot(left, e21[z]).astype(BF).reshape(16, 16, 2 * K)


def dft4(x):
    (a, b), (c, d), (e, f), (g, h) = x
    s0r, s0i, d0r, d0i = a + e, b + f, a - e, b - f
    s1r, s1i, d1r, d1i = c + g, d + h, c - g, d - h
    return (
        (s0r + s1r, s0i + s1i),
        (d0r + d1i, d0i - d1r),
        (s0r - s1r, s0i - s1i),
        (d0r - d1i, d0i + d1r),
    )


def expand_right(row_form):
    n = row_form.shape[-1] // 2
    r, i = row_form[:, :n], row_form[:, n:]
    return jnp.concatenate(
        [jnp.concatenate([r, i], 1), jnp.concatenate([-i, r], 1)], 0
    )


VMEM = pltpu.VMEM


def lead_kernel(pos_hbm, sig_hbm, w_hbm, *rest):
    p2hi, p2lo, d, w43, e21 = rest[:5]
    pos, sig, w, ax_c, ax_s, by_c, by_s, t0, t1, c0, mm, wsem, ssem = rest[5:]
    own_z, own_x = lax.axis_index("z"), lax.axis_index("x")
    child = (own_z // 2, own_z % 2, own_x // 2, own_x % 2)

    pos_copy = pltpu.make_async_copy(pos_hbm, pos, wsem.at[4])
    pos_copy.start()
    w_copies = [
        pltpu.make_async_copy(w_hbm.at[i, :, child[i]], w.at[i], wsem.at[i])
        for i in range(4)
    ]
    for i in (3, 2, 1, 0):
        w_copies[i].start()
    quarter = sig.shape[1] // 4
    s_copies = [
        pltpu.make_async_copy(
            sig_hbm.at[:, pl.ds(i * quarter, quarter), :],
            sig.at[:, pl.ds(i * quarter, quarter), :],
            ssem.at[i],
        )
        for i in range(4)
    ]
    for c in s_copies:
        c.start()

    pos_copy.wait()
    wave = lax.broadcasted_iota(jnp.int32, (SIDE, 1), 0) - SIDE // 2

    def factors(i, _):
        lanes = pl.ds(pl.multiple_of(i * 512, 512), 512)
        xc, xs = sincos(wave * pos[0:1, lanes])
        ax_c[:, lanes] = xc * (1.0 / 16.0)
        ax_s[:, lanes] = xs * (1.0 / 16.0)
        yc, ys = sincos(wave * pos[1:2, lanes])
        by_c[:, lanes] = yc
        by_s[:, lanes] = ys
        return 0

    lax.fori_loop(0, pos.shape[1] // 512, factors, 0)

    row = lax.broadcasted_iota(jnp.int32, (K, K), 0)
    col = lax.broadcasted_iota(jnp.int32, (K, K), 1)
    kx, ky = row // 64, row // 16 % 4
    hx, hy = row // 4 % 4, row % 4
    source = (hx * 4 + kx) * 16 + hy * 4 + ky
    pick = jnp.where(source == col, 1.0, 0.0).astype(BF)

    def row_form(level, r):
        return jnp.concatenate([w[level, r, 0], w[level, r, 1]], 1)

    w_copies[3].wait()
    upper = jnp.concatenate(
        [dot(pick, row_form(3, r)).astype(BF) for r in range(2)], 0
    )
    w_copies[2].wait()
    for r3 in range(2):
        w43[pl.ds(r3 * 512, 512), :] = dot(upper, expand_right(row_form(2, r3))).astype(BF)
    w_copies[1].wait()
    w_copies[0].wait()
    lower = jnp.concatenate([row_form(1, r) for r in range(2)], 0)
    for r1 in range(2):
        both = dot(lower, expand_right(row_form(0, r1))).astype(BF)
        for r2 in range(2):
            e21[r1 * 2 + r2] = expand_right(both[r2 * K : (r2 + 1) * K])

    composites(mm, w43, e21, range(4))

    def build(table, m):
        lanes = slice(m * EB, (m + 1) * EB)
        bc, bs = by_c[:, lanes], by_s[:, lanes]
        for wx in range(SIDE):
            ac, as_ = ax_c[wx : wx + 1, lanes], ax_s[wx : wx + 1, lanes]
            table[wx * 16 : wx * 16 + 16, 0:EB] = (ac * bc - as_ * bs).astype(BF)
            table[wx * 16 : wx * 16 + 16, EB : 2 * EB] = (as_ * bc + ac * bs).astype(BF)

    def multiply(table, m):
        sr = sig[0, m * EB : (m + 1) * EB, :]
        si = sig[1, m * EB : (m + 1) * EB, :]
        right = jnp.concatenate(
            [jnp.concatenate([sr, si], 1), jnp.concatenate([si, -sr], 1)], 0
        )
        c0[m] = dot(table[...], right)

    def along_x(my, part):
        for i in range(part * 8, part * 8 + 8):
            rows = slice(i * 8, i * 8 + 8)
            for half in range(2):
                re_at = slice(half * 128, half * 128 + 128)
                im_at = slice(COLS + half * 128, COLS + half * 128 + 128)
                x = [
                    (c0[my * 4 + mx, rows, re_at], c0[my * 4 + mx, rows, im_at])
                    for mx in range(4)
                ]
                for kx_, (re, im) in enumerate(dft4(x)):
                    c0[my * 4 + kx_, rows, re_at] = re
                    c0[my * 4 + kx_, rows, im_at] = im

    def along_y(kx_, part):
        for i in range(part * 4, part * 4 + 4):
            rows = slice(i * 16, i * 16 + 16)
            low = slice(K + i * 16, K + i * 16 + 16)
            for half in range(2):
                re_at = slice(half * 128, half * 128 + 128)
                im_at = slice(COLS + half * 128, COLS + half * 128 + 128)
                x = [
                    (c0[my * 4 + kx_, rows, re_at], c0[my * 4 + kx_, rows, im_at])
                    for my in range(4)
                ]
                for ky_, (re, im) in enumerate(dft4(x)):
                    re = (re * 0.25).astype(BF)
                    im = (im * 0.25).astype(BF)
                    cls = kx_ * 4 + ky_
                    d[cls, rows, re_at] = re
                    d[cls, rows, im_at] = im
                    d[cls, low, re_at] = -im
                    d[cls, low, im_at] = re

    def apply(cls):
        rows = slice(cls * 16, cls * 16 + 16)
        out = dot(mm[cls].reshape(K // 4, 2 * K), d[cls]).astype(BF).reshape(4, 16, 2 * COLS)
        p2hi[:, rows, :] = out[0:2]
        p2lo[:, rows, :] = out[2:4]

    tables = (t0, t1)
    build(t0, 0)
    for m in range(BOXES):
        if m % 4 == 0:
            s_copies[m // 4].wait()
        if m + 1 < BOXES:
            build(tables[(m + 1) % 2], m + 1)
        multiply(tables[m % 2], m)
        if m >= 4:
            along_x(m // 4 - 1, m % 4)
    for part in range(4):
        along_x(3, part)
    for part in range(4):
        along_y(0, part)
    for cls in range(16):
        if cls < 12:
            along_y(cls // 4 + 1, cls % 4)
        apply(cls)


def vm(n):
    return [pl.BlockSpec(memory_space=VMEM)] * n


def shaped(*dims, dtype=BF):
    return jax.ShapeDtypeStruct(dims, dtype)


def rest_kernel(d, w43, e21, *refs):
    q1u, q1w, qmw, qmu, own, mm = refs
    composites(mm, w43, e21, range(4, 16))
    for cls in range(16):
        rows = slice(cls * 16, cls * 16 + 16)
        out = dot(mm[cls].reshape(3 * K // 4, 2 * K), d[cls]).astype(BF)
        out = out.reshape(3, 4, 16, 2 * COLS)
        q1u[:, rows, :] = out[0, 0:2]
        q1w[:, rows, :] = out[0, 2:4]
        qmw[:, rows, :] = out[1, 0:2]
        qmu[:, rows, :] = out[1, 2:4]
        own[:, rows, :] = out[2]


def lead(positions, signal, weights):
    ne = positions.shape[1]
    hbm = pl.BlockSpec(memory_space=pltpu.HBM)
    far = pl.pallas_call(
        lead_kernel,
        out_shape=[shaped(2, K, 2 * COLS)] * 2
        + [shaped(16, 2 * K, 2 * COLS), shaped(4 * K, 2 * K), shaped(4, 2 * K, 2 * K)],
        in_specs=[hbm] * 3,
        out_specs=vm(5),
        scratch_shapes=[
            VMEM(positions.shape, jnp.int32),
            VMEM(signal.shape, BF),
            VMEM((4, 2, 2, K, K), BF),
        ]
        + [VMEM((SIDE, ne), F32)] * 4
        + [VMEM((K, 2 * EB), BF)] * 2
        + [
            VMEM((BOXES, K, 2 * COLS), F32),
            VMEM((16, 4, 16, 2 * K), BF),
            pltpu.SemaphoreType.DMA((5,)),
            pltpu.SemaphoreType.DMA((4,)),
        ],
        compiler_params=pltpu.CompilerParams(vmem_limit_bytes=LEAD_MIB << 20),
        cost_estimate=pl.CostEstimate(
            flops=8_000_000_000, transcendentals=0, bytes_accessed=12 << 20
        ),
        name="lead",
    )(*(pltpu.with_memory_space_constraint(a, pltpu.HBM) for a in (positions, signal, weights)))
    p2hi, p2lo, d, w43, e21 = far
    near = pl.pallas_call(
        rest_kernel,
        out_shape=[shaped(n, K, 2 * COLS) for n in (2, 2, 2, 2, 4)],
        in_specs=vm(3),
        out_specs=vm(5),
        scratch_shapes=[VMEM((16, 12, 16, 2 * K), BF)],
        compiler_params=pltpu.CompilerParams(vmem_limit_bytes=30 << 20),
        cost_estimate=pl.CostEstimate(
            flops=3_000_000_000, transcendentals=0, bytes_accessed=12 << 20
        ),
        name="rest",
    )(d, w43, e21)
    return p2hi, p2lo, *near


def steer_kernel(pos, out, table):
    r = lax.broadcasted_iota(jnp.int32, (SIDE, 1), 0)
    n = pos.shape[-1]
    u, v = pos[0, 0:1, :], pos[1, 0:1, :]
    for kx in range(4):
        ac, as_ = sincos((r // 4 * 4 + kx - 8) * u)
        ac, as_ = ac * (1.0 / 16.0), as_ * (1.0 / 16.0)
        for ky in range(4):
            bc, bs = sincos((r % 4 * 4 + ky - 8) * v)
            rows = pl.ds((kx * 4 + ky) * 16, 16)
            table[rows, :] = ac * bc - as_ * bs
            table[pl.ds((kx * 4 + ky) * 16 + K, 16), :] = as_ * bc + ac * bs
    for i in range(n // 128):
        for j in range(2 * K // 128):
            block = table[pl.ds(j * 128, 128), pl.ds(i * 128, 128)]
            out[pl.ds(i * 128, 128), pl.ds(j * 128, 128)] = block.T.astype(BF)


def steer(directions):
    n = directions.shape[-1]
    return pl.pallas_call(
        steer_kernel,
        out_shape=shaped(n, 2 * K),
        in_specs=vm(1),
        out_specs=vm(1)[0],
        scratch_shapes=[VMEM((2 * K, n), F32)],
        cost_estimate=pl.CostEstimate(
            flops=1_500_000_000, transcendentals=0, bytes_accessed=1 << 20
        ),
        compiler_params=pltpu.CompilerParams(vmem_limit_bytes=16 << 20),
        name="steer",
    )(directions)


def added(*terms):
    total = terms[0].astype(F32)
    for t in terms[1:]:
        total = total + t.astype(F32)
    return total


def call(kernel, shapes, *args):
    return pl.pallas_call(
        kernel,
        out_shape=shapes,
        in_specs=vm(len(args)),
        out_specs=vm(len(shapes)),
        compiler_params=pltpu.CompilerParams(vmem_limit_bytes=24 << 20),
    )(*args)


def merge_kernel(mine, received, *outs):
    if len(outs) == 1:
        outs[0][...] = added(mine[...], received[...]).astype(BF)
    else:
        for i, o in enumerate(outs):
            o[...] = added(mine[i], received[i]).astype(BF)


def sum_far_kernel(own, g1, gm, lo, hi):
    s = added(own[0], g1[0], gm[...]).astype(BF)
    lo[...] = s[: K // 2]
    hi[...] = s[K // 2 :]


def sum_near_kernel(own, g1u, gmb, g1w, gmu, tlo, thi, u1, um, s0):
    h = K // 2
    one = added(own[1], g1u[1], gmb[...])
    u1[0:h] = (one[:h] + tlo[...].astype(F32)).astype(BF)
    u1[h:] = one[h:].astype(BF)
    other = added(own[2], g1w[0], gmu[0])
    um[0:h] = other[:h].astype(BF)
    um[h:] = (other[h:] + thi[...].astype(F32)).astype(BF)
    s0[...] = added(own[3], g1w[1], gmu[1])


def total_kernel(s0, v1, vm_, z):
    z[...] = added(s0[...], v1[...], vm_[...]).astype(BF)


def beam_kernel(offsets, table, *rest):
    parts = rest[: len(offsets)]
    out, buf, sem = rest[-3:]
    y = lax.axis_index("dir")
    n = table.shape[0] // 2
    copies = []
    for i, offset in enumerate(offsets):
        right = expand_right(parts[i][...])
        column = pl.multiple_of(jnp.bitwise_and(y + offset, 3) * COLS, COLS)
        for r in range(2):
            slot = len(copies) % 2
            if len(copies) >= 2:
                copies[-2].wait()
            b = dot(table[pl.ds(r * n, n), :], right).astype(BF)
            buf[slot, 0] = b[:, :COLS]
            buf[slot, 1] = b[:, COLS:]
            copies.append(
                pltpu.make_async_copy(
                    buf.at[slot],
                    out.at[:, 0, pl.ds(r * n, n), pl.ds(column, COLS)],
                    sem.at[slot],
                )
            )
            copies[-1].start()
    for c in copies[-2:]:
        c.wait()


def beams(offsets, table, parts, previous, shape):
    n = table.shape[0]
    hbm = pl.BlockSpec(memory_space=pltpu.HBM)
    extra = [] if previous is None else [previous]
    return pl.pallas_call(
        lambda *refs: beam_kernel(offsets, *refs),
        out_shape=jax.ShapeDtypeStruct(shape, BF),
        in_specs=vm(1 + len(parts)) + [hbm] * len(extra),
        out_specs=hbm,
        scratch_shapes=[
            VMEM((2, 2, n // 2, COLS), BF),
            pltpu.SemaphoreType.DMA((2,)),
        ],
        input_output_aliases={} if previous is None else {1 + len(parts): 0},
        cost_estimate=pl.CostEstimate(
            flops=2_000_000_000, transcendentals=0, bytes_accessed=1 << 20
        ),
        compiler_params=pltpu.CompilerParams(vmem_limit_bytes=24 << 20),
        name="beams",
    )(table, *parts, *extra)


def ring(step, first):
    pairs = []
    for z in range(4):
        for x in range(4):
            along_z = ((z + step) % 4) * 4 + x
            along_x = z * 4 + (x + step) % 4
            core0, core1 = (along_z, along_x) if first else (along_x, along_z)
            pairs.append((z * 4 + x, core0))
            pairs.append((16 + z * 4 + x, 16 + core1))
    return pairs


def local(signal, positions, weights, directions):
    along = ("freq", "z", "x")

    def major(a, step):
        return lax.ppermute(a, along, ring(step, True))

    def minor(a, step):
        return lax.ppermute(a, along, ring(step, False))

    def across(a, step):
        return lax.ppermute(a, "dir", [(i, (i + step) % 4) for i in range(4)])

    def compute():
        p2hi, p2lo, q1u, q1w, qmw, qmu, own = lead(positions, signal, weights)
        table = steer(directions)
        block = shaped(K, 2 * COLS)
        rhi, rlo = major(p2hi, -1), major(p2lo, 1)
        gmu, g1u = major(qmu, -1), major(q1u, 1)
        wma, wmb = call(merge_kernel, [block, block], qmw, rhi)
        (w1,) = call(merge_kernel, [shaped(2, K, 2 * COLS)], q1w, rlo)
        gma, g1w, gmb = major(wma, -1), major(w1, 1), major(wmb, -1)
        half = shaped(K // 2, 2 * COLS)
        lo, hi = call(sum_far_kernel, [half, half], own, g1u, gma)
        tlo, thi = minor(lo, 1), minor(hi, -1)
        u1, um, s0 = call(
            sum_near_kernel,
            [block, block, shaped(K, 2 * COLS, dtype=F32)],
            own, g1u, gmb, g1w, gmu, tlo, thi,
        )
        v1, v_m = minor(u1, 1), minor(um, -1)
        (zz,) = call(total_kernel, [block], s0, v1, v_m)
        y1, ym, y2 = across(zz, 1), across(zz, -1), across(zz, 2)
        shape = (2, 1, directions.shape[2], signal.shape[2] * 4)
        result = beams((0,), table, (zz,), None, shape)
        result = beams((3,), table, (y1,), result, shape)
        result = beams((1,), table, (ym,), result, shape)
        return beams((2,), table, (y2,), result, shape)

    return compute()


def solution(mesh):
    split = Mesh(mesh.devices.reshape(2, 4, 4, 4), ("freq", "dir", "z", "x"))
    ap = ("z", "x")
    in_specs = (P(None, ap, ("freq", "dir")), P(None, ap), P(), P(None, ap, "dir"))
    out_specs = P(None, ap, "dir", "freq")
    return jax.shard_map(
        local, mesh=split, in_specs=in_specs, out_specs=out_specs, check_vma=False
    )
```
